256 devices in a mesh: row: 16 (over z, y_hi), col: 4 (over x), depth: 4 (over y_lo, core).
Axes of the slice: x: 4, y: 4 (y_hi: 2, y_lo: 2; y = y_hi * 2 + y_lo), z: 8, core: 2. Of those that a mesh axis runs over, the one named last changes fastest.
Arguments:
- pair: bfloat16 [768, 768, 128], P('row', 'col'), may hold values from -6 to 6
- ln_gain: float32 [128], replicated, may hold values from 0.1 to 1.9
- ln_shift: float32 [128], replicated, may hold values from -3 to 3
- proj_weight: bfloat16 [128, 512], replicated, may hold values from -0.5 to 0.5
- proj_bias: float32 [512], replicated, may hold values from -3 to 3
- gate_weight: bfloat16 [128, 128], replicated, may hold values from -0.5 to 0.5
- gate_bias: float32 [128], replicated, may hold values from -3 to 3
- out_gain: float32 [128], replicated, may hold values from 0.1 to 1.9
- out_shift: float32 [128], replicated, may hold values from -3 to 3
- out_weight: bfloat16 [128, 128], replicated, may hold values from -0.5 to 0.5
- out_bias: float32 [128], replicated, may hold values from -3 to 3
Outputs:
- update: bfloat16 [768, 768, 128], P('row', 'col')
The draws below stay inside these ranges and needn't reach their ends.
All inputs are finite; a program needn't handle non-finite values.
Results may differ from the reference program's by a relative error of at most 0.0051.
Values may be sent and summed in bfloat16 or wider, within the bound.
A program may use at most 128 MiB of HBM per device.

```python
import jax
import jax.numpy as jnp
from jax import lax

C = 128
HID = 128
RES = 768


def block_levels(rng, dims, split, low, largest):
    level, own = 1.0, jax.random.fold_in(rng, 6)
    for position, blocks in split:
        heights = jnp.exp(jax.random.uniform(jax.random.fold_in(own, position), (blocks,), jnp.float32, low / len(split), largest / len(split)))
        level = level * jnp.repeat(heights, dims[position] // blocks).reshape([-1 if axis == position else 1 for axis in range(len(dims))])
    return level


def gaussian(key, shape, scale, limit, split=(), kind=jnp.bfloat16):
    result = scale * jax.random.normal(key, shape, jnp.float32)
    if split:
        result = result * block_levels(key, shape, split, -0.22, 0.18)
    return jnp.clip(result, -limit, limit).astype(kind)


def setup_inputs(seed: int = 0) -> dict:
    key_of = jax.random.split(jax.random.key(seed), 12)
    pair = gaussian(key_of[0], (RES, RES, C), 1.0, 6.0, ((0, 16), (1, 4)))
    ln_gain = jnp.clip(1.0 + 0.18 * jax.random.normal(key_of[1], (C,), jnp.float32), 0.1, 1.9)
    ln_shift = gaussian(key_of[2], (C,), 0.5, 3.0, (), jnp.float32)
    proj_weight = gaussian(key_of[3], (C, 4 * HID), C ** -0.5, 0.5)
    proj_bias = gaussian(key_of[4], (4 * HID,), 0.5, 3.0, (), jnp.float32)
    gate_weight = gaussian(key_of[5], (C, C), C ** -0.5, 0.5)
    gate_bias = gaussian(key_of[6], (C,), 0.5, 3.0, (), jnp.float32)
    out_gain = jnp.clip(1.0 + 0.18 * jax.random.normal(key_of[7], (HID,), jnp.float32), 0.1, 1.9)
    out_shift = gaussian(key_of[8], (HID,), 0.5, 3.0, (), jnp.float32)
    out_weight = gaussian(key_of[9], (HID, C), HID ** -0.5, 0.5)
    out_bias = gaussian(key_of[10], (C,), 0.5, 3.0, (), jnp.float32)
    return {"pair": pair, "ln_gain": ln_gain, "ln_shift": ln_shift, "proj_weight": proj_weight, "proj_bias": proj_bias, "gate_weight": gate_weight, "gate_bias": gate_bias, "out_gain": out_gain, "out_shift": out_shift, "out_weight": out_weight, "out_bias": out_bias}


def layer_norm(values, gain, shift):
    centre = lax.optimization_barrier(jnp.mean(values, axis=-1, keepdims=True))
    centred = values - centre
    spread = lax.optimization_barrier(jnp.mean(centred * centred, axis=-1, keepdims=True))
    return centred * lax.rsqrt(spread + 1e-05) * gain + shift

def reference(pair, ln_gain, ln_shift, proj_weight, proj_bias, gate_weight, gate_bias, out_gain, out_shift, out_weight, out_bias):
    hidden = proj_weight.shape[1] // 4
    normed = layer_norm(pair.astype(jnp.float32), ln_gain, ln_shift).astype(jnp.bfloat16)
    flat = normed.reshape(-1, C)
    mixed = jnp.dot(flat, proj_weight, preferred_element_type=jnp.float32) + proj_bias
    left = (jax.nn.sigmoid(mixed[:, :hidden]) * mixed[:, hidden:2 * hidden]).astype(jnp.bfloat16)
    right = (jax.nn.sigmoid(mixed[:, 2 * hidden:3 * hidden]) * mixed[:, 3 * hidden:]).astype(jnp.bfloat16)
    gate = jax.nn.sigmoid(jnp.dot(flat, gate_weight, preferred_element_type=jnp.float32) + gate_bias)
    left = left.reshape(RES, RES, hidden).astype(jnp.float32)
    right = right.reshape(RES, RES, hidden).astype(jnp.float32)
    triangle = jnp.einsum('ikc,jkc->ijc', left, right)
    tri_normed = layer_norm(triangle, out_gain, out_shift).astype(jnp.bfloat16)
    projected = jnp.dot(tri_normed.reshape(-1, hidden), out_weight, preferred_element_type=jnp.float32) + out_bias
    return (gate * projected).reshape(RES, RES, C).astype(jnp.bfloat16)
```

```python
import functools

import jax
import jax.numpy as jnp
from jax import lax
from jax.experimental import pallas as pl
from jax.experimental.pallas import tpu as pltpu
from jax.sharding import PartitionSpec as P

F32 = jnp.float32
BF16 = jnp.bfloat16
EPS = 1e-05
NT = (((1,), (1,)), ((), ()))
TN = (((0,), (0,)), ((), ()))


def remote(src, dst, send_sem, recv_sem, row, col, depth):
    return pltpu.make_async_remote_copy(
        src_ref=src,
        dst_ref=dst,
        send_sem=send_sem,
        recv_sem=recv_sem,
        device_id=(row, col, depth),
        device_id_type=pl.DeviceIdType.MESH,
    )


def kernel(
    pair,
    ln_gain,
    ln_shift,
    proj_weight,
    proj_bias,
    gate_weight,
    gate_bias,
    out_gain,
    out_shift,
    out_weight,
    out_bias,
    out,
    wt,
    bt,
    normed,
    gate,
    stage,
    sbuf,
    rbuf,
    left,
    ring,
    tsend,
    trecv,
    wide,
    x_send,
    x_recv,
    r_send,
    r_recv,
    t_send,
    t_recv,
    o_send,
    o_recv,
):
    row = lax.axis_index("row")
    x = lax.axis_index("col")
    d = lax.axis_index("depth")
    z = row // 2
    yh = row % 2
    yl = d // 2
    core = d % 2
    me = x * 2 + yh

    barrier = pltpu.get_barrier_semaphore()

    def greet(p, carry):
        prow = z * 2 + p // 16
        pcol = (p // 4) % 4
        pd = p % 4
        other = jnp.logical_or(prow != row, jnp.logical_or(pcol != x, pd != d))

        @pl.when(other)
        def _():
            pl.semaphore_signal(
                barrier, inc=1, device_id=(prow, pcol, pd), device_id_type=pl.DeviceIdType.MESH
            )

        return carry

    lax.fori_loop(0, 32, greet, 0)
    up = (row + 2) % 16
    down = (row + 14) % 16
    for nrow in (up, down):
        pl.semaphore_signal(
            barrier, inc=1, device_id=(nrow, x, d), device_id_type=pl.DeviceIdType.MESH
        )

    for b in range(4):
        wt[b * 128 : (b + 1) * 128, :] = (
            proj_weight[:, b * 128 : (b + 1) * 128].astype(F32).T.astype(BF16)
        )
        bt[b * 128 : (b + 1) * 128, :] = jnp.broadcast_to(
            proj_bias[:, b * 128 : (b + 1) * 128], (128, 128)
        ).T
    first = pl.multiple_of(d * 32, 32)
    wsel = jnp.concatenate([wt[pl.ds(first + 128 * b, 32), :] for b in range(4)], axis=0)
    gain = ln_gain[...]
    shift = ln_shift[...]

    def norm_rows(t, carry):
        vals = jnp.concatenate([pair[t], pair[t + 24]], axis=0).astype(F32)
        centred = vals - jnp.mean(vals, axis=-1, keepdims=True)
        spread = jnp.mean(centred * centred, axis=-1, keepdims=True)
        rows = (centred * lax.rsqrt(spread + EPS) * gain + shift).astype(BF16)
        normed[t] = rows[:192]
        normed[t + 24] = rows[192:]
        mixed = lax.dot_general(wsel, rows, NT, preferred_element_type=F32)
        at = pl.ds(pl.multiple_of(t * 32, 32), 32)
        for q in range(3):
            part = [
                mixed[b * 32 : (b + 1) * 32, q * 128 : (q + 1) * 128]
                + bt[pl.ds(first + 128 * b, 32), :]
                for b in range(4)
            ]
            stage[0, q, at, :] = jax.nn.sigmoid(part[2]) * part[3]
            stage[1, q, at, :] = jax.nn.sigmoid(part[0]) * part[1]
        return carry

    lax.fori_loop(0, 24, norm_rows, 0)
    pl.semaphore_wait(barrier, 33)

    def exchange(kind):
        def body(g, carry):
            for q in range(3):
                rows = [
                    stage[kind, q, pl.ds(g * 4 + c, 24, stride=32), :] for c in range(4)
                ]
                sbuf[kind, g, :, q * 128 : (q + 1) * 128] = jnp.concatenate(rows, axis=0).astype(
                    BF16
                )

            @pl.when(g != me)
            def _():
                remote(
                    sbuf.at[kind, g],
                    rbuf.at[kind, me],
                    x_send.at[kind],
                    x_recv.at[kind],
                    z * 2 + g % 2,
                    g // 2,
                    d,
                ).start()

            @pl.when(g == me)
            def _():
                pltpu.make_async_copy(
                    sbuf.at[kind, g], rbuf.at[kind, me], x_recv.at[kind]
                ).start()

            return carry

        lax.fori_loop(0, 8, body, 0)

    def unpack(kind, put):
        low = lax.broadcasted_iota(jnp.int32, (24, 128), 1) < 64
        for u in range(2):
            for y in range(2):
                one = rbuf[kind, 4 * u + y].astype(F32)
                two = rbuf[kind, 4 * u + 2 + y].astype(F32)
                for c in range(4):
                    a = [one[c * 24 : (c + 1) * 24, q * 128 : (q + 1) * 128] for q in range(3)]
                    b = [two[c * 24 : (c + 1) * 24, q * 128 : (q + 1) * 128] for q in range(3)]
                    ra1 = pltpu.roll(a[1], 64, 1)
                    ra2 = pltpu.roll(a[2], 64, 1)
                    rb0 = pltpu.roll(b[0], 64, 1)
                    rb1 = pltpu.roll(b[1], 64, 1)
                    evens = [a[0], jnp.where(low, a[1], rb0), jnp.where(low, rb0, rb1)]
                    odds = [jnp.where(low, ra1, ra2), jnp.where(low, ra2, b[1]), b[2]]
                    for q in range(3):
                        put(c, u, y, q, jnp.concatenate([evens[q], odds[q]], axis=0).astype(BF16))

    def put_ring(c, u, y, q, tile):
        ring[z, c, u, y * 48 : (y + 1) * 48, q * 128 : (q + 1) * 128] = tile

    def put_left(c, u, y, q, tile):
        left[c, u, y * 48 : (y + 1) * 48, q * 128 : (q + 1) * 128] = tile

    def ring_copy(way, step, c):
        held = (z + 8 - step + 1) % 8 if way == 0 else (z + step - 1) % 8
        piece = ring.at[held, c]
        return remote(
            piece,
            piece,
            r_send.at[way, step - 1, c],
            r_recv.at[way, step - 1, c],
            up if way == 0 else down,
            x,
            d,
        )

    def multiply(plane, c):
        total = lax.dot_general(left[c, 0], ring[plane, c, 0], NT, preferred_element_type=F32)
        total += lax.dot_general(left[c, 1], ring[plane, c, 1], NT, preferred_element_type=F32)
        total = total.astype(BF16)
        tsend[plane * 2, c * 48 : (c + 1) * 48, 0:96] = total[:48]
        tsend[plane * 2 + 1, c * 48 : (c + 1) * 48, 0:96] = total[48:]

    def hand_out(plane):
        pcol = plane // 2
        pcore = plane % 2
        slot = d * 8 + me

        def body(n, carry):
            ph = n // 2
            rel = n % 2
            pl_lo = (yl + rel) % 2
            prow = z * 2 + ph
            pd = pl_lo * 2 + pcore
            other = jnp.logical_or(prow != row, jnp.logical_or(pcol != x, pd != d))

            @pl.when(other)
            def _():
                remote(
                    tsend.at[plane * 2 + ph],
                    trecv.at[slot],
                    t_send.at[rel],
                    t_recv.at[0],
                    prow,
                    pcol,
                    pd,
                ).start()

            @pl.when(jnp.logical_not(other))
            def _():
                pltpu.make_async_copy(
                    tsend.at[plane * 2 + ph], trecv.at[slot], t_recv.at[0]
                ).start()

            return carry

        lax.fori_loop(0, 4, body, 0)

    exchange(0)
    exchange(1)
    tsend[...] = jnp.zeros_like(tsend)

    pltpu.make_async_copy(sbuf.at[0], rbuf.at[0], x_recv.at[0]).wait()
    unpack(0, put_ring)
    for c in range(4):
        ring_copy(0, 1, c).start()
        ring_copy(1, 1, c).start()

    mine = pl.ds(pl.multiple_of(core * 96, 96), 96)

    def gate_rows(i, carry):
        gate[i] = jax.nn.sigmoid(
            jnp.dot(normed[i, mine, :], gate_weight[...], preferred_element_type=F32)
            + gate_bias[...]
        )
        return carry

    lax.fori_loop(0, 48, gate_rows, 0)
    pltpu.make_async_copy(sbuf.at[1], rbuf.at[1], x_recv.at[1]).wait()
    unpack(1, put_left)
    for c in range(4):
        multiply(z, c)
    hand_out(z)

    for step in range(1, 5):
        plus = (z + 8 - step) % 8
        minus = (z + step) % 8
        for c in range(4):
            for way in range(2):
                if step < 4 or c // 2 == way:
                    ring_copy(way, step, c).wait_recv()
                    if step < 3 or (step == 3 and c // 2 == way):
                        ring_copy(way, step + 1, c).start()
            multiply(plus, c)
            if step < 4:
                multiply(minus, c)
        hand_out(plus)
        if step < 4:
            hand_out(minus)

    out_gains = jnp.broadcast_to(out_gain[...], (128, 128)).T
    out_shifts = jnp.broadcast_to(out_shift[...], (128, 128)).T
    wide_copy = pltpu.make_async_copy(trecv, trecv, t_recv.at[0])
    wide_copy.wait()

    def widen(s, carry):
        wide[pl.ds(pl.multiple_of(s * 192, 192), 192), :] = trecv[s].astype(F32)
        return carry

    lax.fori_loop(0, 32, widen, 0)

    def finish_row(i):
        vals = wide[pl.ds(i, 128, stride=48), :]
        centred = vals - jnp.mean(vals, axis=0, keepdims=True)
        spread = jnp.mean(centred * centred, axis=0, keepdims=True)
        rows = (centred * lax.rsqrt(spread + EPS) * out_gains + out_shifts).T.astype(BF16)
        projected = (
            jnp.dot(rows[:96], out_weight[...], preferred_element_type=F32) + out_bias[...]
        )
        out[i, mine, :] = (gate[i] * projected).astype(BF16)

    def swap(n):
        part = out.at[pl.ds(n * 12, 12), mine]
        return remote(part, part, o_send.at[n], o_recv.at[n], row, x, yl * 2 + 1 - core)

    for n in range(4):

        def body(k, carry, n=n):
            finish_row(n * 12 + k)
            return carry

        lax.fori_loop(0, 12, body, 0)
        swap(n).start()

    for kind in range(2):
        pltpu.make_async_copy(
            sbuf.at[kind, pl.ds(0, 7)], rbuf.at[kind, pl.ds(0, 7)], x_send.at[kind]
        ).wait()
    for step in range(1, 5):
        for c in range(4):
            for way in range(2):
                if step < 4 or c // 2 == way:
                    ring_copy(way, step, c).wait_send()
    for rel in range(2):
        units = pl.ds(0, 15 if rel == 0 else 16)
        pltpu.make_async_copy(tsend.at[units], trecv.at[units], t_send.at[rel]).wait()
    for n in range(4):
        swap(n).wait()


def per_device(pair, ln_gain, ln_shift, proj_weight, proj_bias, gate_weight, gate_bias, out_gain, out_shift, out_weight, out_bias):
    line = lambda v: v.reshape(1, -1)
    vmem = pl.BlockSpec(memory_space=pltpu.VMEM)
    dma = pltpu.SemaphoreType.DMA
    return pl.pallas_call(
        kernel,
        out_shape=jax.ShapeDtypeStruct(pair.shape, BF16),
        in_specs=[vmem] * 11,
        out_specs=vmem,
        scratch_shapes=[
            pltpu.VMEM((512, 128), BF16),
            pltpu.VMEM((512, 128), F32),
            pltpu.VMEM((48, 192, 128), BF16),
            pltpu.VMEM((48, 96, 128), F32),
            pltpu.VMEM((2, 3, 24 * 32, 128), F32),
            pltpu.VMEM((2, 8, 96, 384), BF16),
            pltpu.VMEM((2, 8, 96, 384), BF16),
            pltpu.VMEM((4, 2, 96, 384), BF16),
            pltpu.VMEM((8, 4, 2, 96, 384), BF16),
            pltpu.VMEM((16, 192, 128), BF16),
            pltpu.VMEM((32, 192, 128), BF16),
            pltpu.VMEM((6144, 128), F32),
            dma((2,)),
            dma((2,)),
            dma((2, 4, 4)),
            dma((2, 4, 4)),
            dma((2,)),
            dma((1,)),
            dma((4,)),
            dma((4,)),
        ],
        compiler_params=pltpu.CompilerParams(
            collective_id=0, has_side_effects=True, vmem_limit_bytes=56 * 1024 * 1024
        ),
    )(
        pair,
        line(ln_gain),
        line(ln_shift),
        proj_weight,
        line(proj_bias),
        gate_weight,
        line(gate_bias),
        line(out_gain),
        line(out_shift),
        out_weight,
        line(out_bias),
    )


def solution(mesh):
    in_specs = (P("row", "col", None),) + (P(),) * 10
    return jax.shard_map(
        per_device, mesh=mesh, in_specs=in_specs, out_specs=P("row", "col", None), check_vma=False
    )
```

```python
import functools

import jax
import jax.numpy as jnp
from jax import lax
from jax.experimental import pallas as pl
from jax.experimental.pallas import tpu as pltpu
from jax.sharding import PartitionSpec as P

F32 = jnp.float32
BF16 = jnp.bfloat16
EPS = 1e-05
NT = (((1,), (1,)), ((), ()))
VMEM_MIB = 40


def remote(src, dst, send_sem, recv_sem, row, col, depth):
    return pltpu.make_async_remote_copy(
        src_ref=src,
        dst_ref=dst,
        send_sem=send_sem,
        recv_sem=recv_sem,
        device_id=(row, col, depth),
        device_id_type=pl.DeviceIdType.MESH,
    )


def kernel(
    pair_hbm,
    ln_gain,
    ln_shift,
    proj_weight,
    proj_bias,
    gate_weight,
    gate_bias,
    out_gain,
    out_shift,
    out_weight,
    out_bias,
    out,
    pair,
    wt,
    bt,
    normed,
    gate,
    stage,
    sbuf,
    rbuf,
    left,
    ring,
    tsend,
    trecv,
    wide,
    table,
    p_sem,
    x_send,
    x_recv,
    r_send,
    r_recv,
    h_send,
    h_recv,
    t_send,
    t_recv,
    o_send,
    o_recv,
):
    row = lax.axis_index("row")
    x = lax.axis_index("col")
    d = lax.axis_index("depth")
    z = row // 2
    yh = row % 2
    yl = d // 2
    core = d % 2
    me = x * 2 + yh

    def load(p, half):
        rows = pl.ds(half * 24 + p * 8, 8)
        return pltpu.make_async_copy(pair_hbm.at[rows], pair.at[rows], p_sem.at[p, half])

    for p in range(3):
        for half in range(2):
            load(p, half).start()

    barrier = pltpu.get_barrier_semaphore()

    def greet(p, carry):
        prow = z * 2 + p // 16
        pcol = (p // 4) % 4
        pd = p % 4
        other = jnp.logical_or(prow != row, jnp.logical_or(pcol != x, pd != d))

        @pl.when(other)
        def _():
            pl.semaphore_signal(
                barrier, inc=1, device_id=(prow, pcol, pd), device_id_type=pl.DeviceIdType.MESH
            )

        return carry

    lax.fori_loop(0, 32, greet, 0)
    up = (row + 2) % 16
    down = (row + 14) % 16
    for nrow in (up, down):
        pl.semaphore_signal(
            barrier, inc=1, device_id=(nrow, x, d), device_id_type=pl.DeviceIdType.MESH
        )

    for b in range(4):
        wt[b * 128 : (b + 1) * 128, :] = (
            proj_weight[:, b * 128 : (b + 1) * 128].astype(F32).T.astype(BF16)
        )
        bt[b * 128 : (b + 1) * 128, :] = jnp.broadcast_to(
            proj_bias[:, b * 128 : (b + 1) * 128], (128, 128)
        ).T
    first = pl.multiple_of(d * 32, 32)
    wsel = jnp.concatenate([wt[pl.ds(first + 128 * b, 32), :] for b in range(4)], axis=0)
    gain = ln_gain[...]
    shift = ln_shift[...]

    def project(p):
        def body(n, carry):
            t = p * 8 + n
            vals = jnp.concatenate([pair[t], pair[t + 24]], axis=0).astype(F32)
            centred = vals - jnp.mean(vals, axis=-1, keepdims=True)
            spread = jnp.mean(centred * centred, axis=-1, keepdims=True)
            rows = (centred * lax.rsqrt(spread + EPS) * gain + shift).astype(BF16)
            normed[t] = rows[:192]
            normed[t + 24] = rows[192:]
            mixed = lax.dot_general(wsel, rows, NT, preferred_element_type=F32)
            at = pl.ds(pl.multiple_of(n * 32, 32), 32)
            for q in range(3):
                cut = [
                    mixed[b * 32 : (b + 1) * 32, q * 128 : (q + 1) * 128]
                    + bt[pl.ds(first + 128 * b, 32), :]
                    for b in range(4)
                ]
                stage[0, p, q, at, :] = jax.nn.sigmoid(cut[2]) * cut[3]
                stage[1, p, q, at, :] = jax.nn.sigmoid(cut[0]) * cut[1]
            return carry

        for half in range(2):
            load(p, half).wait()
        lax.fori_loop(0, 8, body, 0, unroll=2)

    def exchange(kind, p):
        def body(g, carry):
            for q in range(3):
                rows = [
                    stage[kind, p, q, pl.ds(g * 4 + c, 8, stride=32), :] for c in range(4)
                ]
                sbuf[kind, p, g, :, q * 128 : (q + 1) * 128] = jnp.concatenate(
                    rows, axis=0
                ).astype(BF16)

            @pl.when(g != me)
            def _():
                remote(
                    sbuf.at[kind, p, g],
                    rbuf.at[kind, p, me],
                    x_send.at[kind, p],
                    x_recv.at[kind, p],
                    z * 2 + g % 2,
                    g // 2,
                    d,
                ).start()

            @pl.when(g == me)
            def _():
                pltpu.make_async_copy(
                    sbuf.at[kind, p, g], rbuf.at[kind, p, me], x_recv.at[kind, p]
                ).start()

            return carry

        lax.fori_loop(0, 8, body, 0)

    low = lax.broadcasted_iota(jnp.int32, (32, 128), 1) < 64

    def unpack(kind, p, put):
        pltpu.make_async_copy(sbuf.at[kind, p], rbuf.at[kind, p], x_recv.at[kind, p]).wait()
        for u in range(2):
            for y in range(2):
                one = rbuf[kind, p, 4 * u + y].astype(F32)
                two = rbuf[kind, p, 4 * u + 2 + y].astype(F32)
                a = [one[:, q * 128 : (q + 1) * 128] for q in range(3)]
                b = [two[:, q * 128 : (q + 1) * 128] for q in range(3)]
                ra1 = pltpu.roll(a[1], 64, 1)
                ra2 = pltpu.roll(a[2], 64, 1)
                rb0 = pltpu.roll(b[0], 64, 1)
                rb1 = pltpu.roll(b[1], 64, 1)
                evens = [a[0], jnp.where(low, a[1], rb0), jnp.where(low, rb0, rb1)]
                odds = [jnp.where(low, ra1, ra2), jnp.where(low, ra2, b[1]), b[2]]
                for c in range(4):
                    at = slice(c * 8, c * 8 + 8)
                    for q in range(3):
                        put(
                            c, u, y, slice(q * 128, q * 128 + 128),
                            jnp.concatenate([evens[q][at], odds[q][at]], axis=0).astype(BF16),
                        )

    def unpack_right(p):
        def put(c, u, y, lanes, tile):
            ring[z, p, c, u, y * 16 : y * 16 + 16, lanes] = tile

        unpack(0, p, put)

    def unpack_left(p):
        def put(c, u, y, lanes, tile):
            left[c, u, p * 32 + y * 16 : p * 32 + y * 16 + 16, lanes] = tile

        unpack(1, p, put)

    def ring_copy(way, step, p):
        held = (z + 8 - step + 1) % 8 if way == 0 else (z + step - 1) % 8
        to = up if way == 0 else down
        if step < 4:
            piece = ring.at[held, p]
            return remote(
                piece, piece, r_send.at[way, step - 1, p], r_recv.at[way, step - 1, p], to, x, d
            )
        piece = ring.at[held, p, pl.ds(way * 2, 2)]
        return remote(piece, piece, h_send.at[way, p], h_recv.at[way, p], to, x, d)

    lane_group = lax.broadcasted_iota(jnp.int32, (96, 128), 1) // 32

    def multiply(plane, p):
        tile = None
        for c in range(4):
            total = None
            for u in range(2):
                rows = ring[plane, p, c, u]
                term = lax.dot_general(
                    left[c, u],
                    jnp.concatenate([rows] * 4, axis=0),
                    NT,
                    preferred_element_type=F32,
                )
                total = term if total is None else total + term
            tile = total if tile is None else jnp.where(lane_group == c, total, tile)
        tile = tile.astype(BF16)
        for ph in range(2):
            tsend[(plane * 3 + p) * 2 + ph] = jnp.concatenate(
                [tile[k * 32 + ph * 16 : k * 32 + ph * 16 + 16] for k in range(3)], axis=0
            )
        hand_out(plane, p)

    def hand_out(plane, p):
        pcol = plane // 2
        pcore = plane % 2
        slot = d * 8 + me
        for ph in range(2):
            for rel in range(2):
                prow = z * 2 + ph
                pd = ((yl + rel) % 2) * 2 + pcore
                unit = tsend.at[(plane * 3 + p) * 2 + ph]
                copy = remote(
                    unit, trecv.at[p, slot], t_send.at[rel], t_recv.at[p], prow, pcol, pd
                )
                if rel == 1:
                    copy.start()
                    continue
                other = jnp.logical_or(prow != row, jnp.logical_or(pcol != x, pd != d))

                @pl.when(other)
                def _():
                    copy.start()

                @pl.when(jnp.logical_not(other))
                def _():
                    pltpu.make_async_copy(unit, trecv.at[p, slot], t_recv.at[p]).start()

    def start_ring(p):
        unpack_right(p)
        ring_copy(0, 1, p).start()
        ring_copy(1, 1, p).start()

    project(0)
    pl.semaphore_wait(barrier, 33)
    exchange(0, 0)
    project(1)
    exchange(0, 1)
    start_ring(0)
    project(2)
    exchange(0, 2)
    start_ring(1)
    for p in range(3):
        exchange(1, p)
    start_ring(2)

    mine = pl.ds(pl.multiple_of(core * 96, 96), 96)

    def gate_rows(n, carry):
        at = pl.ds(n * 4, 4)
        logits = (
            jnp.dot(
                normed[at, mine, :].reshape(384, 128),
                gate_weight[...],
                preferred_element_type=F32,
            )
            + gate_bias[...]
        )
        gate[at] = jax.nn.sigmoid(logits).reshape(4, 96, 128)
        return carry

    lax.fori_loop(0, 12, gate_rows, 0)
    table[0] = jnp.broadcast_to(out_gain[...], (128, 128)).T
    table[1] = jnp.broadcast_to(out_shift[...], (128, 128)).T
    table[2] = out_weight[...].astype(F32)

    for p in range(3):
        unpack_left(p)

    for step in range(1, 5):
        plus = (z + 8 - step) % 8
        minus = (z + step) % 8
        for p in range(3):
            for way in range(2):
                ring_copy(way, step, p).wait_recv()
                if step < 4:
                    ring_copy(way, step + 1, p).start()
            if step == 1:
                multiply(z, p)
            multiply(plus, p)
            if step < 4:
                multiply(minus, p)

    def regroup(n):
        return jnp.concatenate(
            [table[n, pl.ds(c, 32, stride=4), :] for c in range(4)], axis=0
        )

    gains = regroup(0)
    shifts = regroup(1)
    weight = regroup(2).astype(BF16)
    group = lax.broadcasted_iota(jnp.int32, (32, 128), 1) // 32

    def swap(p, k):
        part = out.at[:, pl.ds(pl.multiple_of(core * 96 + k * 24 + p * 8, 8), 8), :]
        return remote(
            part, part, o_send.at[p, k], o_recv.at[p, k], row, x, yl * 2 + 1 - core
        )

    for p in range(3):
        pltpu.make_async_copy(trecv.at[p], trecv.at[p], t_recv.at[p]).wait()

        def widen(s, carry, p=p):
            at = pl.ds(pl.multiple_of(s * 192, 192), 192)
            wide[at, :] = trecv[p, pl.ds(s * 4, 4)].reshape(192, 128).astype(F32)
            return carry

        lax.fori_loop(0, 8, widen, 0, unroll=2)

        def finish(g, carry, p=p):
            from_row = [wide[pl.ds(g * 4 + i, 32, stride=48), :] for i in range(4)]
            blocks = []
            for c in range(4):
                block = None
                for i in range(4):
                    turn = (32 * (i - c)) % 128
                    moved = pltpu.roll(from_row[i], turn, 1) if turn else from_row[i]
                    block = moved if block is None else jnp.where(group == i, moved, block)
                blocks.append(block)
            vals = jnp.concatenate(blocks, axis=0)
            centred = vals - jnp.mean(vals, axis=0, keepdims=True)
            spread = jnp.mean(centred * centred, axis=0, keepdims=True)
            rows = (centred * lax.rsqrt(spread + EPS) * gains + shifts).T.astype(BF16)
            projected = jnp.dot(rows, weight, preferred_element_type=F32) + out_bias[...]
            for i in range(4):
                line = ((g % 4) // 2) * 24 + (g // 4) * 8 + (g % 2) * 4 + i
                for k in range(4):
                    j = k * 24 + p * 8
                    value = (
                        gate[line, j : j + 8, :]
                        * projected[i * 32 + k * 8 : i * 32 + k * 8 + 8]
                    )
                    out[line, pl.ds(pl.multiple_of(core * 96 + j, 8), 8), :] = value.astype(BF16)
            return carry

        lax.fori_loop(0, 12, finish, 0, unroll=2)
        for k in range(4):
            swap(p, k).start()

    for kind in range(2):
        for p in range(3):
            pltpu.make_async_copy(
                sbuf.at[kind, p, pl.ds(0, 7)], rbuf.at[kind, p, pl.ds(0, 7)], x_send.at[kind, p]
            ).wait()
    for step in range(1, 5):
        for p in range(3):
            for way in range(2):
                ring_copy(way, step, p).wait_send()
    for rel in range(2):
        units = tsend.at[pl.ds(0, 45 if rel == 0 else 48)]
        pltpu.make_async_copy(units, units, t_send.at[rel]).wait()
    for p in range(3):
        for k in range(4):
            swap(p, k).wait()


def per_device(
    pair,
    ln_gain,
    ln_shift,
    proj_weight,
    proj_bias,
    gate_weight,
    gate_bias,
    out_gain,
    out_shift,
    out_weight,
    out_bias,
):
    line = lambda v: v.reshape(1, -1)
    vmem = pl.BlockSpec(memory_space=pltpu.VMEM)
    dma = pltpu.SemaphoreType.DMA
    return pl.pallas_call(
        kernel,
        out_shape=jax.ShapeDtypeStruct(pair.shape, BF16),
        in_specs=[pl.BlockSpec(memory_space=pl.ANY)] + [vmem] * 10,
        out_specs=vmem,
        scratch_shapes=[
            pltpu.VMEM((48, 192, 128), BF16),
            pltpu.VMEM((512, 128), BF16),
            pltpu.VMEM((512, 128), F32),
            pltpu.VMEM((48, 192, 128), BF16),
            pltpu.VMEM((48, 96, 128), F32),
            pltpu.VMEM((2, 3, 3, 256, 128), F32),
            pltpu.VMEM((2, 3, 8, 32, 384), BF16),
            pltpu.VMEM((2, 3, 8, 32, 384), BF16),
            pltpu.VMEM((4, 2, 96, 384), BF16),
            pltpu.VMEM((8, 3, 4, 2, 32, 384), BF16),
            pltpu.VMEM((48, 48, 128), BF16),
            pltpu.VMEM((3, 32, 48, 128), BF16),
            pltpu.VMEM((1536, 128), F32),
            pltpu.VMEM((3, 128, 128), F32),
            dma((3, 2)),
            dma((2, 3)),
            dma((2, 3)),
            dma((2, 3, 3)),
            dma((2, 3, 3)),
            dma((2, 3)),
            dma((2, 3)),
            dma((2,)),
            dma((3,)),
            dma((3, 4)),
            dma((3, 4)),
        ],
        compiler_params=pltpu.CompilerParams(
            collective_id=0, has_side_effects=True, vmem_limit_bytes=VMEM_MIB * 1024 * 1024
        ),
    )(
        pair,
        line(ln_gain),
        line(ln_shift),
        proj_weight,
        line(proj_bias),
        gate_weight,
        line(gate_bias),
        line(out_gain),
        line(out_shift),
        out_weight,
        line(out_bias),
    )


def solution(mesh):
    in_specs = (P("row", "col", None),) + (P(),) * 10
    return jax.shard_map(
        per_device, mesh=mesh, in_specs=in_specs, out_specs=P("row", "col", None), check_vma=False
    )
```

```python
import functools

import jax
import jax.numpy as jnp
from jax import lax
from jax.experimental import pallas as pl
from jax.experimental.pallas import tpu as pltpu
from jax.sharding import PartitionSpec as P

F32 = jnp.float32
BF16 = jnp.bfloat16
EPS = 1e-05
NT = (((1,), (1,)), ((), ()))
VMEM_MIB = 50
UNROLL = 4


def remote(src, dst, send_sem, recv_sem, row, col, depth):
    return pltpu.make_async_remote_copy(
        src_ref=src,
        dst_ref=dst,
        send_sem=send_sem,
        recv_sem=recv_sem,
        device_id=(row, col, depth),
        device_id_type=pl.DeviceIdType.MESH,
    )


def kernel(*refs):
    work(refs[0], refs[1:11], refs[12:22], refs[11], *refs[12:])


def work(
    pair_hbm,
    sources,
    params,
    out,
    ln_gain,
    ln_shift,
    proj_weight,
    proj_bias,
    gate_weight,
    gate_bias,
    out_gain,
    out_shift,
    out_weight,
    out_bias,
    pair,
    wt,
    bt,
    normed,
    gate,
    stage,
    sbuf,
    rbuf,
    left,
    ring,
    tsend,
    trecv,
    wide,
    table,
    normal,
    w_sem,
    p_sem,
    x_send,
    x_recv,
    r_send,
    r_recv,
    h_send,
    h_recv,
    t_send,
    t_recv,
    o_send,
    o_recv,
):
    row = lax.axis_index("row")
    x = lax.axis_index("col")
    d = lax.axis_index("depth")
    z = row // 2
    yh = row % 2
    yl = d // 2
    core = d % 2
    me = x * 2 + yh

    def load(p, half):
        rows = pl.ds(half * 24 + p * 8, 8)
        return pltpu.make_async_copy(pair_hbm.at[rows], pair.at[rows], p_sem.at[p, half])

    for half in range(2):
        load(0, half).start()
    fetches = [
        pltpu.make_async_copy(src, dst, w_sem.at[n])
        for n, (src, dst) in enumerate(zip(sources, params))
    ]
    for fetch in fetches:
        fetch.start()
    for p in range(1, 3):
        for half in range(2):
            load(p, half).start()

    barrier = pltpu.get_barrier_semaphore()

    def greet(p, carry):
        prow = z * 2 + p // 16
        pcol = (p // 4) % 4
        pd = p % 4
        other = jnp.logical_or(prow != row, jnp.logical_or(pcol != x, pd != d))

        @pl.when(other)
        def _():
            pl.semaphore_signal(
                barrier, inc=1, device_id=(prow, pcol, pd), device_id_type=pl.DeviceIdType.MESH
            )

        return carry

    lax.fori_loop(0, 32, greet, 0)
    up = (row + 2) % 16
    down = (row + 14) % 16
    for nrow in (up, down):
        pl.semaphore_signal(
            barrier, inc=1, device_id=(nrow, x, d), device_id_type=pl.DeviceIdType.MESH
        )

    for fetch in fetches:
        fetch.wait()

    for b in range(4):
        wt[b * 128 : (b + 1) * 128, :] = (
            proj_weight[:, b * 128 : (b + 1) * 128].astype(F32).T.astype(BF16)
        )
        bt[b * 128 : (b + 1) * 128, :] = jnp.broadcast_to(
            proj_bias[:, b * 128 : (b + 1) * 128], (128, 128)
        ).T
    first = pl.multiple_of(d * 32, 32)
    wsel = jnp.concatenate([wt[pl.ds(first + 128 * b, 32), :] for b in range(4)], axis=0)
    gain = ln_gain[...]
    shift = ln_shift[...]

    def project(p):
        def body(n, carry):
            t = p * 8 + n
            vals = jnp.concatenate([pair[t], pair[t + 24]], axis=0).astype(F32)
            centred = vals - jnp.mean(vals, axis=-1, keepdims=True)
            spread = jnp.mean(centred * centred, axis=-1, keepdims=True)
            rows = (centred * lax.rsqrt(spread + EPS) * gain + shift).astype(BF16)
            normed[t] = rows[:192]
            normed[t + 24] = rows[192:]
            mixed = lax.dot_general(wsel, rows, NT, preferred_element_type=F32)
            at = pl.ds(pl.multiple_of(n * 32, 32), 32)
            for q in range(3):
                cut = [
                    mixed[b * 32 : (b + 1) * 32, q * 128 : (q + 1) * 128]
                    + bt[pl.ds(first + 128 * b, 32), :]
                    for b in range(4)
                ]
                stage[0, p, q, at, :] = jax.nn.sigmoid(cut[2]) * cut[3]
                stage[1, p, q, at, :] = jax.nn.sigmoid(cut[0]) * cut[1]
            return carry

        for half in range(2):
            load(p, half).wait()
        lax.fori_loop(0, 8, body, 0, unroll=2)

    def exchange(kind, p):
        def body(g, carry):
            for q in range(3):
                rows = [
                    stage[kind, p, q, pl.ds(g * 4 + c, 8, stride=32), :] for c in range(4)
                ]
                sbuf[kind, p, g, :, q * 128 : (q + 1) * 128] = jnp.concatenate(
                    rows, axis=0
                ).astype(BF16)

            @pl.when(g != me)
            def _():
                remote(
                    sbuf.at[kind, p, g],
                    rbuf.at[kind, p, me],
                    x_send.at[kind, p],
                    x_recv.at[kind, p],
                    z * 2 + g % 2,
                    g // 2,
                    d,
                ).start()

            @pl.when(g == me)
            def _():
                pltpu.make_async_copy(
                    sbuf.at[kind, p, g], rbuf.at[kind, p, me], x_recv.at[kind, p]
                ).start()

            return carry

        lax.fori_loop(0, 8, body, 0)

    low = lax.broadcasted_iota(jnp.int32, (32, 128), 1) < 64

    def unpack(kind, p, put):
        pltpu.make_async_copy(sbuf.at[kind, p], rbuf.at[kind, p], x_recv.at[kind, p]).wait()
        for u in range(2):
            for y in range(2):
                one = rbuf[kind, p, 4 * u + y].astype(F32)
                two = rbuf[kind, p, 4 * u + 2 + y].astype(F32)
                a = [one[:, q * 128 : (q + 1) * 128] for q in range(3)]
                b = [two[:, q * 128 : (q + 1) * 128] for q in range(3)]
                ra1 = pltpu.roll(a[1], 64, 1)
                ra2 = pltpu.roll(a[2], 64, 1)
                rb0 = pltpu.roll(b[0], 64, 1)
                rb1 = pltpu.roll(b[1], 64, 1)
                evens = [a[0], jnp.where(low, a[1], rb0), jnp.where(low, rb0, rb1)]
                odds = [jnp.where(low, ra1, ra2), jnp.where(low, ra2, b[1]), b[2]]
                for c in range(4):
                    at = slice(c * 8, c * 8 + 8)
                    for q in range(3):
                        put(
                            c, u, y, slice(q * 128, q * 128 + 128),
                            jnp.concatenate([evens[q][at], odds[q][at]], axis=0).astype(BF16),
                        )

    def unpack_right(p):
        def put(c, u, y, lanes, tile):
            ring[z, p, c, u, y * 16 : y * 16 + 16, lanes] = tile

        unpack(0, p, put)

    def unpack_left(p):
        def put(c, u, y, lanes, tile):
            left[c, u, p * 32 + y * 16 : p * 32 + y * 16 + 16, lanes] = tile

        unpack(1, p, put)

    def ring_copy(way, step, p):
        held = (z + 8 - step + 1) % 8 if way == 0 else (z + step - 1) % 8
        to = up if way == 0 else down
        if step < 4:
            piece = ring.at[held, p]
            return remote(
                piece, piece, r_send.at[way, step - 1, p], r_recv.at[way, step - 1, p], to, x, d
            )
        piece = ring.at[held, p, pl.ds(way * 2, 2)]
        return remote(piece, piece, h_send.at[way, p], h_recv.at[way, p], to, x, d)

    lane_group = lax.broadcasted_iota(jnp.int32, (96, 128), 1) // 32

    def multiply(plane, p):
        tile = None
        for c in range(4):
            total = None
            for u in range(2):
                rows = ring[plane, p, c, u]
                term = lax.dot_general(
                    left[c, u],
                    jnp.concatenate([rows] * 4, axis=0),
                    NT,
                    preferred_element_type=F32,
                )
                total = term if total is None else total + term
            tile = total if tile is None else jnp.where(lane_group == c, total, tile)
        tile = tile.astype(BF16)
        for ph in range(2):
            tsend[(plane * 3 + p) * 2 + ph] = jnp.concatenate(
                [tile[k * 32 + ph * 16 : k * 32 + ph * 16 + 16] for k in range(3)], axis=0
            )
        hand_out(plane, p)

    def hand_out(plane, p):
        pcol = plane // 2
        pcore = plane % 2
        slot = d * 8 + me
        for ph in range(2):
            for rel in range(2):
                prow = z * 2 + ph
                pd = ((yl + rel) % 2) * 2 + pcore
                unit = tsend.at[(plane * 3 + p) * 2 + ph]
                copy = remote(
                    unit, trecv.at[p, slot], t_send.at[rel], t_recv.at[p], prow, pcol, pd
                )
                if rel == 1:
                    copy.start()
                    continue
                other = jnp.logical_or(prow != row, jnp.logical_or(pcol != x, pd != d))

                @pl.when(other)
                def _():
                    copy.start()

                @pl.when(jnp.logical_not(other))
                def _():
                    pltpu.make_async_copy(unit, trecv.at[p, slot], t_recv.at[p]).start()

    def start_ring(p):
        unpack_right(p)
        ring_copy(0, 1, p).start()
        ring_copy(1, 1, p).start()

    project(0)
    pl.semaphore_wait(barrier, 33)
    exchange(0, 0)
    project(1)
    exchange(0, 1)
    project(2)
    exchange(0, 2)
    start_ring(0)
    start_ring(1)
    for p in range(3):
        exchange(1, p)
    start_ring(2)

    mine = pl.ds(pl.multiple_of(core * 96, 96), 96)

    def gate_rows(n, carry):
        at = pl.ds(n * 4, 4)
        logits = (
            jnp.dot(
                normed[at, mine, :].reshape(384, 128),
                gate_weight[...],
                preferred_element_type=F32,
            )
            + gate_bias[...]
        )
        gate[at] = jax.nn.sigmoid(logits).reshape(4, 96, 128)
        return carry

    lax.fori_loop(0, 12, gate_rows, 0)
    table[0] = jnp.broadcast_to(out_gain[...], (128, 128)).T
    table[1] = jnp.broadcast_to(out_shift[...], (128, 128)).T
    table[2] = out_weight[...].astype(F32)

    for p in range(3):
        unpack_left(p)

    for step in range(1, 5):
        plus = (z + 8 - step) % 8
        minus = (z + step) % 8
        for p in range(3):
            for way in range(2):
                ring_copy(way, step, p).wait_recv()
                if step < 4:
                    ring_copy(way, step + 1, p).start()
            if step == 1:
                multiply(z, p)
            multiply(plus, p)
            if step < 4:
                multiply(minus, p)

    def regroup(n):
        return jnp.concatenate(
            [table[n, pl.ds(c, 32, stride=4), :] for c in range(4)], axis=0
        )

    gains = regroup(0)
    shifts = regroup(1)
    weight = regroup(2).astype(BF16)
    group = lax.broadcasted_iota(jnp.int32, (32, 128), 1) // 32

    def swap(p, k):
        part = out.at[:, pl.ds(pl.multiple_of(core * 96 + k * 24 + p * 8, 8), 8), :]
        return remote(
            part, part, o_send.at[p, k], o_recv.at[p, k], row, x, yl * 2 + 1 - core
        )

    for p in range(3):
        pltpu.make_async_copy(trecv.at[p], trecv.at[p], t_recv.at[p]).wait()

        def widen(s, carry, p=p):
            at = pl.ds(pl.multiple_of(s * 192, 192), 192)
            wide[at, :] = trecv[p, pl.ds(s * 4, 4)].reshape(192, 128).astype(F32)
            return carry

        lax.fori_loop(0, 8, widen, 0, unroll=2)

        def finish(g, carry, p=p):
            from_row = [wide[pl.ds(g * 4 + i, 32, stride=48), :] for i in range(4)]
            blocks = []
            for c in range(4):
                block = None
                for i in range(4):
                    turn = (32 * (i - c)) % 128
                    moved = pltpu.roll(from_row[i], turn, 1) if turn else from_row[i]
                    block = moved if block is None else jnp.where(group == i, moved, block)
                blocks.append(block)
            vals = jnp.concatenate(blocks, axis=0)
            centred = vals - jnp.mean(vals, axis=0, keepdims=True)
            spread = jnp.mean(centred * centred, axis=0, keepdims=True)
            rows = (centred * lax.rsqrt(spread + EPS) * gains + shifts).astype(BF16)
            normal[pl.ds(pl.multiple_of(g * 128, 128), 128), :] = rows.T
            return carry

        lax.fori_loop(0, 12, finish, 0, unroll=UNROLL)

        def apply(g, carry, p=p):
            rows = normal[pl.ds(pl.multiple_of(g * 256, 256), 256), :]
            projected = jnp.dot(rows, weight, preferred_element_type=F32) + out_bias[...]
            for i in range(8):
                line = (g % 2) * 24 + (g // 2) * 8 + i
                for k in range(4):
                    j = k * 24 + p * 8
                    value = (
                        gate[line, j : j + 8, :]
                        * projected[i * 32 + k * 8 : i * 32 + k * 8 + 8]
                    )
                    out[line, pl.ds(pl.multiple_of(core * 96 + j, 8), 8), :] = value.astype(BF16)
            return carry

        lax.fori_loop(0, 6, apply, 0, unroll=2)
        for k in range(4):
            swap(p, k).start()

    for kind in range(2):
        for p in range(3):
            pltpu.make_async_copy(
                sbuf.at[kind, p, pl.ds(0, 7)], rbuf.at[kind, p, pl.ds(0, 7)], x_send.at[kind, p]
            ).wait()
    for step in range(1, 5):
        for p in range(3):
            for way in range(2):
                ring_copy(way, step, p).wait_send()
    for rel in range(2):
        units = tsend.at[pl.ds(0, 45 if rel == 0 else 48)]
        pltpu.make_async_copy(units, units, t_send.at[rel]).wait()
    for p in range(3):
        for k in range(4):
            swap(p, k).wait()


def per_device(
    pair,
    ln_gain,
    ln_shift,
    proj_weight,
    proj_bias,
    gate_weight,
    gate_bias,
    out_gain,
    out_shift,
    out_weight,
    out_bias,
):
    line = lambda v: v.reshape(1, -1)
    operands = (
        pair,
        line(ln_gain),
        line(ln_shift),
        proj_weight,
        line(proj_bias),
        gate_weight,
        line(gate_bias),
        line(out_gain),
        line(out_shift),
        out_weight,
        line(out_bias),
    )
    vmem = pl.BlockSpec(memory_space=pltpu.VMEM)
    dma = pltpu.SemaphoreType.DMA
    return pl.pallas_call(
        kernel,
        out_shape=jax.ShapeDtypeStruct(pair.shape, BF16),
        in_specs=[pl.BlockSpec(memory_space=pl.ANY)] * 11,
        out_specs=vmem,
        scratch_shapes=[
            *[pltpu.VMEM(v.shape, v.dtype) for v in operands[1:]],
            pltpu.VMEM((48, 192, 128), BF16),
            pltpu.VMEM((512, 128), BF16),
            pltpu.VMEM((512, 128), F32),
            pltpu.VMEM((48, 192, 128), BF16),
            pltpu.VMEM((48, 96, 128), F32),
            pltpu.VMEM((2, 3, 3, 256, 128), F32),
            pltpu.VMEM((2, 3, 8, 32, 384), BF16),
            pltpu.VMEM((2, 3, 8, 32, 384), BF16),
            pltpu.VMEM((4, 2, 96, 384), BF16),
            pltpu.VMEM((8, 3, 4, 2, 32, 384), BF16),
            pltpu.VMEM((48, 48, 128), BF16),
            pltpu.VMEM((3, 32, 48, 128), BF16),
            pltpu.VMEM((1536, 128), F32),
            pltpu.VMEM((3, 128, 128), F32),
            pltpu.VMEM((1536, 128), BF16),
            dma((10,)),
            dma((3, 2)),
            dma((2, 3)),
            dma((2, 3)),
            dma((2, 3, 3)),
            dma((2, 3, 3)),
            dma((2, 3)),
            dma((2, 3)),
            dma((2,)),
            dma((3,)),
            dma((3, 4)),
            dma((3, 4)),
        ],
        compiler_params=pltpu.CompilerParams(
            collective_id=0, has_side_effects=True, vmem_limit_bytes=VMEM_MIB * 1024 * 1024
        ),
    )(*[pltpu.with_memory_space_constraint(v, pltpu.HBM) for v in operands])


def solution(mesh):
    in_specs = (P("row", "col", None),) + (P(),) * 10
    return jax.shard_map(
        per_device, mesh=mesh, in_specs=in_specs, out_specs=P("row", "col", None), check_vma=False
    )
```

```python
import functools

import jax
import jax.numpy as jnp
from jax import lax
from jax.experimental import pallas as pl
from jax.experimental.pallas import tpu as pltpu
from jax.sharding import PartitionSpec as P

F32 = jnp.float32
BF16 = jnp.bfloat16
EPS = 1e-05
NT = (((1,), (1,)), ((), ()))
VMEM_MIB = 50
UNROLL = 6
ORDER = (1, 2, 0)


def remote(src, dst, send_sem, recv_sem, row, col, depth):
    return pltpu.make_async_remote_copy(
        src_ref=src,
        dst_ref=dst,
        send_sem=send_sem,
        recv_sem=recv_sem,
        device_id=(row, col, depth),
        device_id_type=pl.DeviceIdType.MESH,
    )


def kernel(*refs):
    work(refs[0], refs[1:11], refs[12:22], refs[11], *refs[12:])


def work(
    pair_hbm,
    sources,
    params,
    out,
    ln_gain,
    ln_shift,
    proj_weight,
    proj_bias,
    gate_weight,
    gate_bias,
    out_gain,
    out_shift,
    out_weight,
    out_bias,
    pair,
    wt,
    bt,
    normed,
    gate,
    stage,
    sbuf,
    rbuf,
    left,
    ring,
    tsend,
    trecv,
    wide,
    table,
    normal,
    raw,
    raw_in,
    w_sem,
    p_sem,
    w_send,
    w_recv,
    v_send,
    v_recv,
    x_send,
    x_recv,
    r_send,
    r_recv,
    h_send,
    h_recv,
    t_send,
    t_recv,
    o_send,
    o_recv,
):
    row = lax.axis_index("row")
    x = lax.axis_index("col")
    d = lax.axis_index("depth")
    z = row // 2
    yh = row % 2
    yl = d // 2
    core = d % 2
    me = x * 2 + yh

    def load(p, half):
        rows = pl.ds(half * 24 + p * 8, 8)
        return pltpu.make_async_copy(pair_hbm.at[rows], pair.at[rows], p_sem.at[p, half])

    for half in range(2):
        load(0, half).start()
    fetches = [
        pltpu.make_async_copy(src, dst, w_sem.at[n])
        for n, (src, dst) in enumerate(zip(sources, params))
    ]
    for fetch in fetches:
        fetch.start()
    for p in range(1, 3):
        for half in range(2):
            load(p, half).start()

    barrier = pltpu.get_barrier_semaphore()

    def greet(p, carry):
        prow = z * 2 + p // 16
        pcol = (p // 4) % 4
        pd = p % 4
        other = jnp.logical_or(prow != row, jnp.logical_or(pcol != x, pd != d))

        @pl.when(other)
        def _():
            pl.semaphore_signal(
                barrier, inc=1, device_id=(prow, pcol, pd), device_id_type=pl.DeviceIdType.MESH
            )

        return carry

    lax.fori_loop(0, 32, greet, 0)
    up = (row + 2) % 16
    down = (row + 14) % 16
    for nrow in (up, down):
        pl.semaphore_signal(
            barrier, inc=1, device_id=(nrow, x, d), device_id_type=pl.DeviceIdType.MESH
        )

    for fetch in fetches:
        fetch.wait()

    for b in range(4):
        wt[b * 128 : (b + 1) * 128, :] = (
            proj_weight[:, b * 128 : (b + 1) * 128].astype(F32).T.astype(BF16)
        )
        bt[b * 128 : (b + 1) * 128, :] = jnp.broadcast_to(
            proj_bias[:, b * 128 : (b + 1) * 128], (128, 128)
        ).T
    first = pl.multiple_of(d * 32, 32)
    wsel = jnp.concatenate([wt[pl.ds(first + 128 * b, 32), :] for b in range(4)], axis=0)
    gain = ln_gain[...]
    shift = ln_shift[...]

    def project(p):
        def body(n, carry):
            t = p * 8 + n
            vals = jnp.concatenate([pair[t], pair[t + 24]], axis=0).astype(F32)
            centred = vals - jnp.mean(vals, axis=-1, keepdims=True)
            spread = jnp.mean(centred * centred, axis=-1, keepdims=True)
            rows = (centred * lax.rsqrt(spread + EPS) * gain + shift).astype(BF16)
            normed[t] = rows[:192]
            normed[t + 24] = rows[192:]
            mixed = lax.dot_general(wsel, rows, NT, preferred_element_type=F32)
            at = pl.ds(pl.multiple_of(n * 32, 32), 32)
            for q in range(3):
                cut = [
                    mixed[b * 32 : (b + 1) * 32, q * 128 : (q + 1) * 128]
                    + bt[pl.ds(first + 128 * b, 32), :]
                    for b in range(4)
                ]
                stage[0, p, q, at, :] = jax.nn.sigmoid(cut[2]) * cut[3]
                stage[1, p, q, at, :] = jax.nn.sigmoid(cut[0]) * cut[1]
            return carry

        for half in range(2):
            load(p, half).wait()
        lax.fori_loop(0, 8, body, 0, unroll=2)

    def pack(kind, p):
        def body(g, carry):
            for q in range(3):
                rows = [
                    stage[kind, p, q, pl.ds(g * 4 + c, 8, stride=32), :] for c in range(4)
                ]
                sbuf[kind, p, g, :, q * 128 : (q + 1) * 128] = jnp.concatenate(
                    rows, axis=0
                ).astype(BF16)
            return carry

        lax.fori_loop(0, 8, body, 0, unroll=2)

    def spread(source, target, send_sem, recv_sem):
        def body(g, carry):
            @pl.when(g != me)
            def _():
                remote(
                    source.at[g], target.at[me], send_sem, recv_sem, z * 2 + g % 2, g // 2, d
                ).start()

            @pl.when(g == me)
            def _():
                pltpu.make_async_copy(source.at[g], target.at[me], recv_sem).start()

            return carry

        lax.fori_loop(0, 8, body, 0)

    def exchange(kind, p):
        spread(sbuf.at[kind, p], rbuf.at[kind, p], x_send.at[kind, p], x_recv.at[kind, p])

    def raw_copy(way):
        to = up if way == 0 else down
        return remote(sbuf.at[0, 0], raw.at[way], w_send.at[way], w_recv.at[way], to, x, d)

    def raw_spread(way):
        raw_copy(way).wait_recv()
        spread(raw.at[way], raw_in.at[way], v_send.at[way], v_recv.at[way])

    low = lax.broadcasted_iota(jnp.int32, (32, 128), 1) < 64

    def unpack(source, recv_sem, put):
        pltpu.make_async_copy(source, source, recv_sem).wait()
        for u in range(2):
            for y in range(2):
                one = source[4 * u + y].astype(F32)
                two = source[4 * u + 2 + y].astype(F32)
                a = [one[:, q * 128 : (q + 1) * 128] for q in range(3)]
                b = [two[:, q * 128 : (q + 1) * 128] for q in range(3)]
                ra1 = pltpu.roll(a[1], 64, 1)
                ra2 = pltpu.roll(a[2], 64, 1)
                rb0 = pltpu.roll(b[0], 64, 1)
                rb1 = pltpu.roll(b[1], 64, 1)
                evens = [a[0], jnp.where(low, a[1], rb0), jnp.where(low, rb0, rb1)]
                odds = [jnp.where(low, ra1, ra2), jnp.where(low, ra2, b[1]), b[2]]
                for c in range(4):
                    at = slice(c * 8, c * 8 + 8)
                    for q in range(3):
                        put(
                            c, u, y, slice(q * 128, q * 128 + 128),
                            jnp.concatenate([evens[q][at], odds[q][at]], axis=0).astype(BF16),
                        )

    def unpack_right(p):
        def put(c, u, y, lanes, tile):
            ring[z, p, c, u, y * 16 : y * 16 + 16, lanes] = tile

        unpack(rbuf.at[0, p], x_recv.at[0, p], put)

    def unpack_raw(way):
        plane = (z + 7) % 8 if way == 0 else (z + 1) % 8

        def put(c, u, y, lanes, tile):
            ring[plane, 0, c, u, y * 16 : y * 16 + 16, lanes] = tile

        unpack(raw_in.at[way], v_recv.at[way], put)

    def unpack_left(p):
        def put(c, u, y, lanes, tile):
            left[c, u, p * 32 + y * 16 : p * 32 + y * 16 + 16, lanes] = tile

        unpack(rbuf.at[1, p], x_recv.at[1, p], put)

    def ring_copy(way, step, p):
        held = (z + 8 - step + 1) % 8 if way == 0 else (z + step - 1) % 8
        to = up if way == 0 else down
        if step < 4:
            piece = ring.at[held, p]
            return remote(
                piece, piece, r_send.at[way, step - 1, p], r_recv.at[way, step - 1, p], to, x, d
            )
        piece = ring.at[held, p, pl.ds(way * 2, 2)]
        return remote(piece, piece, h_send.at[way, p], h_recv.at[way, p], to, x, d)

    lane_group = lax.broadcasted_iota(jnp.int32, (96, 128), 1) // 32

    def multiply(plane, p):
        tile = None
        for c in range(4):
            total = None
            for u in range(2):
                rows = ring[plane, p, c, u]
                term = lax.dot_general(
                    left[c, u],
                    jnp.concatenate([rows] * 4, axis=0),
                    NT,
                    preferred_element_type=F32,
                )
                total = term if total is None else total + term
            tile = total if tile is None else jnp.where(lane_group == c, total, tile)
        tile = tile.astype(BF16)
        for ph in range(2):
            tsend[(plane * 3 + p) * 2 + ph] = jnp.concatenate(
                [tile[k * 32 + ph * 16 : k * 32 + ph * 16 + 16] for k in range(3)], axis=0
            )
        hand_out(plane, p)

    def hand_out(plane, p):
        pcol = plane // 2
        pcore = plane % 2
        slot = d * 8 + me
        for ph in range(2):
            for rel in range(2):
                prow = z * 2 + ph
                pd = ((yl + rel) % 2) * 2 + pcore
                unit = tsend.at[(plane * 3 + p) * 2 + ph]
                copy = remote(
                    unit, trecv.at[p, slot], t_send.at[rel], t_recv.at[p], prow, pcol, pd
                )
                if rel == 1:
                    copy.start()
                    continue
                other = jnp.logical_or(prow != row, jnp.logical_or(pcol != x, pd != d))

                @pl.when(other)
                def _():
                    copy.start()

                @pl.when(jnp.logical_not(other))
                def _():
                    pltpu.make_async_copy(unit, trecv.at[p, slot], t_recv.at[p]).start()

    def start_ring(p):
        ring_copy(0, 1, p).start()
        ring_copy(1, 1, p).start()

    project(0)
    pack(0, 0)
    project(1)
    pack(0, 1)
    pl.semaphore_wait(barrier, 33)
    exchange(0, 0)
    raw_copy(0).start()
    raw_copy(1).start()
    exchange(0, 1)
    project(2)
    pack(0, 2)
    exchange(0, 2)
    for p in range(3):
        pack(1, p)
    unpack_right(1)
    start_ring(1)
    raw_spread(0)
    raw_spread(1)
    unpack_right(2)
    start_ring(2)
    for p in range(3):
        exchange(1, p)
    unpack_right(0)

    mine = pl.ds(pl.multiple_of(core * 96, 96), 96)

    def gate_rows(n, carry):
        at = pl.ds(n * 4, 4)
        logits = (
            jnp.dot(
                normed[at, mine, :].reshape(384, 128),
                gate_weight[...],
                preferred_element_type=F32,
            )
            + gate_bias[...]
        )
        gate[at] = jax.nn.sigmoid(logits).reshape(4, 96, 128)
        return carry

    lax.fori_loop(0, 12, gate_rows, 0)
    table[0] = jnp.broadcast_to(out_gain[...], (128, 128)).T
    table[1] = jnp.broadcast_to(out_shift[...], (128, 128)).T
    table[2] = out_weight[...].astype(F32)

    for step in range(1, 5):
        plus = (z + 8 - step) % 8
        minus = (z + step) % 8
        for p in ORDER:
            for way in range(2):
                if step == 1 and p == 0:
                    unpack_raw(way)
                else:
                    ring_copy(way, step, p).wait_recv()
                if step < 4:
                    ring_copy(way, step + 1, p).start()
            if step > 1:
                multiply(plus, p)
                if step < 4:
                    multiply(minus, p)
        if step == 1:
            for p in range(3):
                unpack_left(p)
            for p in range(3):
                multiply(z, p)
                multiply(plus, p)
                multiply(minus, p)

    def regroup(n):
        return jnp.concatenate(
            [table[n, pl.ds(c, 32, stride=4), :] for c in range(4)], axis=0
        )

    gains = regroup(0)
    shifts = regroup(1)
    weight = regroup(2).astype(BF16)
    group = lax.broadcasted_iota(jnp.int32, (32, 128), 1) // 32

    def swap(p, k):
        part = out.at[:, pl.ds(pl.multiple_of(core * 96 + k * 24 + p * 8, 8), 8), :]
        return remote(
            part, part, o_send.at[p, k], o_recv.at[p, k], row, x, yl * 2 + 1 - core
        )

    for p in ORDER:
        pltpu.make_async_copy(trecv.at[p], trecv.at[p], t_recv.at[p]).wait()

        def widen(s, carry, p=p):
            at = pl.ds(pl.multiple_of(s * 192, 192), 192)
            wide[at, :] = trecv[p, pl.ds(s * 4, 4)].reshape(192, 128).astype(F32)
            return carry

        lax.fori_loop(0, 8, widen, 0, unroll=2)

        def finish(g, carry, p=p):
            from_row = [wide[pl.ds(g * 4 + i, 32, stride=48), :] for i in range(4)]
            blocks = []
            for c in range(4):
                block = None
                for i in range(4):
                    turn = (32 * (i - c)) % 128
                    moved = pltpu.roll(from_row[i], turn, 1) if turn else from_row[i]
                    block = moved if block is None else jnp.where(group == i, moved, block)
                blocks.append(block)
            vals = jnp.concatenate(blocks, axis=0)
            centred = vals - jnp.mean(vals, axis=0, keepdims=True)
            spread = jnp.mean(centred * centred, axis=0, keepdims=True)
            rows = (centred * lax.rsqrt(spread + EPS) * gains + shifts).astype(BF16)
            normal[pl.ds(pl.multiple_of(g * 128, 128), 128), :] = rows.T
            return carry

        lax.fori_loop(0, 12, finish, 0, unroll=UNROLL)

        def apply(g, carry, p=p):
            rows = normal[pl.ds(pl.multiple_of(g * 256, 256), 256), :]
            projected = jnp.dot(rows, weight, preferred_element_type=F32) + out_bias[...]
            for i in range(8):
                line = (g % 2) * 24 + (g // 2) * 8 + i
                for k in range(4):
                    j = k * 24 + p * 8
                    value = (
                        gate[line, j : j + 8, :]
                        * projected[i * 32 + k * 8 : i * 32 + k * 8 + 8]
                    )
                    out[line, pl.ds(pl.multiple_of(core * 96 + j, 8), 8), :] = value.astype(BF16)
            return carry

        lax.fori_loop(0, 6, apply, 0, unroll=2)
        for k in range(4):
            swap(p, k).start()

    for kind in range(2):
        for p in range(3):
            pltpu.make_async_copy(
                sbuf.at[kind, p, pl.ds(0, 7)], rbuf.at[kind, p, pl.ds(0, 7)], x_send.at[kind, p]
            ).wait()
    for way in range(2):
        raw_copy(way).wait_send()
        pltpu.make_async_copy(
            raw.at[way, pl.ds(0, 7)], raw_in.at[way, pl.ds(0, 7)], v_send.at[way]
        ).wait()
    for step in range(1, 5):
        for p in range(3):
            for way in range(2):
                if step > 1 or p > 0:
                    ring_copy(way, step, p).wait_send()
    for rel in range(2):
        units = tsend.at[pl.ds(0, 45 if rel == 0 else 48)]
        pltpu.make_async_copy(units, units, t_send.at[rel]).wait()
    for p in range(3):
        for k in range(4):
            swap(p, k).wait()


def per_device(
    pair,
    ln_gain,
    ln_shift,
    proj_weight,
    proj_bias,
    gate_weight,
    gate_bias,
    out_gain,
    out_shift,
    out_weight,
    out_bias,
):
    line = lambda v: v.reshape(1, -1)
    operands = (
        pair,
        line(ln_gain),
        line(ln_shift),
        proj_weight,
        line(proj_bias),
        gate_weight,
        line(gate_bias),
        line(out_gain),
        line(out_shift),
        out_weight,
        line(out_bias),
    )
    vmem = pl.BlockSpec(memory_space=pltpu.VMEM)
    dma = pltpu.SemaphoreType.DMA
    return pl.pallas_call(
        kernel,
        out_shape=jax.ShapeDtypeStruct(pair.shape, BF16),
        in_specs=[pl.BlockSpec(memory_space=pl.ANY)] * 11,
        out_specs=vmem,
        scratch_shapes=[
            *[pltpu.VMEM(v.shape, v.dtype) for v in operands[1:]],
            pltpu.VMEM((48, 192, 128), BF16),
            pltpu.VMEM((512, 128), BF16),
            pltpu.VMEM((512, 128), F32),
            pltpu.VMEM((48, 192, 128), BF16),
            pltpu.VMEM((48, 96, 128), F32),
            pltpu.VMEM((2, 3, 3, 256, 128), F32),
            pltpu.VMEM((2, 3, 8, 32, 384), BF16),
            pltpu.VMEM((2, 3, 8, 32, 384), BF16),
            pltpu.VMEM((4, 2, 96, 384), BF16),
            pltpu.VMEM((8, 3, 4, 2, 32, 384), BF16),
            pltpu.VMEM((48, 48, 128), BF16),
            pltpu.VMEM((3, 32, 48, 128), BF16),
            pltpu.VMEM((1536, 128), F32),
            pltpu.VMEM((3, 128, 128), F32),
            pltpu.VMEM((1536, 128), BF16),
            pltpu.VMEM((2, 8, 32, 384), BF16),
            pltpu.VMEM((2, 8, 32, 384), BF16),
            dma((10,)),
            dma((3, 2)),
            dma((2,)),
            dma((2,)),
            dma((2,)),
            dma((2,)),
            dma((2, 3)),
            dma((2, 3)),
            dma((2, 3, 3)),
            dma((2, 3, 3)),
            dma((2, 3)),
            dma((2, 3)),
            dma((2,)),
            dma((3,)),
            dma((3, 4)),
            dma((3, 4)),
        ],
        compiler_params=pltpu.CompilerParams(
            collective_id=0, has_side_effects=True, vmem_limit_bytes=VMEM_MIB * 1024 * 1024
        ),
    )(*[pltpu.with_memory_space_constraint(v, pltpu.HBM) for v in operands])


def solution(mesh):
    in_specs = (P("row", "col", None),) + (P(),) * 10
    return jax.shard_map(
        per_device, mesh=mesh, in_specs=in_specs, out_specs=P("row", "col", None), check_vma=False
    )
```

```python
import functools

import jax
import jax.numpy as jnp
from jax import lax
from jax.experimental import pallas as pl
from jax.experimental.pallas import tpu as pltpu
from jax.sharding import PartitionSpec as P

F32 = jnp.float32
BF16 = jnp.bfloat16
EPS = 1e-05
NT = (((1,), (1,)), ((), ()))
VMEM_MIB = 50
UNROLL = 6
ORDER = (1, 2, 0)


def remote(src, dst, send_sem, recv_sem, row, col, depth):
    return pltpu.make_async_remote_copy(
        src_ref=src,
        dst_ref=dst,
        send_sem=send_sem,
        recv_sem=recv_sem,
        device_id=(row, col, depth),
        device_id_type=pl.DeviceIdType.MESH,
    )


def kernel(*refs):
    work(refs[0], refs[1:11], refs[12:22], refs[11], *refs[12:])


def work(
    pair_hbm,
    sources,
    params,
    out,
    ln_gain,
    ln_shift,
    proj_weight,
    proj_bias,
    gate_weight,
    gate_bias,
    out_gain,
    out_shift,
    out_weight,
    out_bias,
    pair,
    wt,
    bt,
    normed,
    gate,
    stage,
    sbuf,
    rbuf,
    left,
    ring,
    tsend,
    trecv,
    wide,
    table,
    normal,
    raw,
    raw_in,
    w_sem,
    p_sem,
    w_send,
    w_recv,
    v_send,
    v_recv,
    x_send,
    x_recv,
    r_send,
    r_recv,
    h_send,
    h_recv,
    t_send,
    t_recv,
    o_send,
    o_recv,
):
    row = lax.axis_index("row")
    x = lax.axis_index("col")
    d = lax.axis_index("depth")
    z = row // 2
    yh = row % 2
    yl = d // 2
    core = d % 2
    me = x * 2 + yh

    def load(p, half):
        rows = pl.ds(half * 24 + p * 8, 8)
        return pltpu.make_async_copy(pair_hbm.at[rows], pair.at[rows], p_sem.at[p, half])

    for half in range(2):
        load(0, half).start()
    fetches = [
        pltpu.make_async_copy(src, dst, w_sem.at[n])
        for n, (src, dst) in enumerate(zip(sources, params))
    ]
    for fetch in fetches:
        fetch.start()
    for p in range(1, 3):
        for half in range(2):
            load(p, half).start()

    barrier = pltpu.get_barrier_semaphore()

    up = (row + 2) % 16
    down = (row + 14) % 16
    greeted = [
        (z * 2 + (yh + a) % 2, (x + b) % 4, (d + e) % 4)
        for b in (2, 1, 3, 0)
        for a in (1, 0)
        for e in (2, 1, 3, 0)
        if a or b or e
    ]
    for device in greeted + [(up, x, d), (down, x, d)]:
        pl.semaphore_signal(
            barrier, inc=1, device_id=device, device_id_type=pl.DeviceIdType.MESH
        )

    for fetch in fetches:
        fetch.wait()

    for b in range(4):
        wt[b * 128 : (b + 1) * 128, :] = (
            proj_weight[:, b * 128 : (b + 1) * 128].astype(F32).T.astype(BF16)
        )
        bt[b * 128 : (b + 1) * 128, :] = jnp.broadcast_to(
            proj_bias[:, b * 128 : (b + 1) * 128], (128, 128)
        ).T
    first = pl.multiple_of(d * 32, 32)
    wsel = jnp.concatenate([wt[pl.ds(first + 128 * b, 32), :] for b in range(4)], axis=0)
    gain = ln_gain[...]
    shift = ln_shift[...]

    def project(p):
        def body(n, carry):
            t = p * 8 + n
            vals = jnp.concatenate([pair[t], pair[t + 24]], axis=0).astype(F32)
            centred = vals - jnp.mean(vals, axis=-1, keepdims=True)
            spread = jnp.mean(centred * centred, axis=-1, keepdims=True)
            rows = (centred * lax.rsqrt(spread + EPS) * gain + shift).astype(BF16)
            normed[t] = rows[:192]
            normed[t + 24] = rows[192:]
            mixed = lax.dot_general(wsel, rows, NT, preferred_element_type=F32)
            at = pl.ds(pl.multiple_of(n * 32, 32), 32)
            for q in range(3):
                cut = [
                    mixed[b * 32 : (b + 1) * 32, q * 128 : (q + 1) * 128]
                    + bt[pl.ds(first + 128 * b, 32), :]
                    for b in range(4)
                ]
                stage[0, p, q, at, :] = jax.nn.sigmoid(cut[2]) * cut[3]
                stage[1, p, q, at, :] = jax.nn.sigmoid(cut[0]) * cut[1]
            return carry

        for half in range(2):
            load(p, half).wait()
        lax.fori_loop(0, 8, body, 0, unroll=2)

    def pack(kind, p):
        def body(g, carry):
            for q in range(3):
                rows = [
                    stage[kind, p, q, pl.ds(g * 4 + c, 8, stride=32), :] for c in range(4)
                ]
                sbuf[kind, p, g, :, q * 128 : (q + 1) * 128] = jnp.concatenate(
                    rows, axis=0
                ).astype(BF16)
            return carry

        lax.fori_loop(0, 8, body, 0, unroll=2)

    def spread(source, target, send_sem, recv_sem):
        for n in (5, 4, 3, 1, 2, 6, 7):
            g = (me + n) % 8
            remote(
                source.at[g], target.at[me], send_sem, recv_sem, z * 2 + g % 2, g // 2, d
            ).start()
        pltpu.make_async_copy(source.at[me], target.at[me], recv_sem).start()

    def exchange(kind, p):
        spread(sbuf.at[kind, p], rbuf.at[kind, p], x_send.at[kind, p], x_recv.at[kind, p])

    def raw_copy(way):
        to = up if way == 0 else down
        return remote(sbuf.at[0, 0], raw.at[way], w_send.at[way], w_recv.at[way], to, x, d)

    def raw_spread(way):
        raw_copy(way).wait_recv()
        spread(raw.at[way], raw_in.at[way], v_send.at[way], v_recv.at[way])

    low = lax.broadcasted_iota(jnp.int32, (32, 128), 1) < 64

    def unpack(source, recv_sem, put):
        pltpu.make_async_copy(source, source, recv_sem).wait()
        for u in range(2):
            for y in range(2):
                one = source[4 * u + y].astype(F32)
                two = source[4 * u + 2 + y].astype(F32)
                a = [one[:, q * 128 : (q + 1) * 128] for q in range(3)]
                b = [two[:, q * 128 : (q + 1) * 128] for q in range(3)]
                ra1 = pltpu.roll(a[1], 64, 1)
                ra2 = pltpu.roll(a[2], 64, 1)
                rb0 = pltpu.roll(b[0], 64, 1)
                rb1 = pltpu.roll(b[1], 64, 1)
                evens = [a[0], jnp.where(low, a[1], rb0), jnp.where(low, rb0, rb1)]
                odds = [jnp.where(low, ra1, ra2), jnp.where(low, ra2, b[1]), b[2]]
                for c in range(4):
                    at = slice(c * 8, c * 8 + 8)
                    for q in range(3):
                        put(
                            c, u, y, slice(q * 128, q * 128 + 128),
                            jnp.concatenate([evens[q][at], odds[q][at]], axis=0).astype(BF16),
                        )

    def unpack_right(p):
        def put(c, u, y, lanes, tile):
            ring[z, p, c, u, y * 16 : y * 16 + 16, lanes] = tile

        unpack(rbuf.at[0, p], x_recv.at[0, p], put)

    def unpack_raw(way):
        plane = (z + 7) % 8 if way == 0 else (z + 1) % 8

        def put(c, u, y, lanes, tile):
            ring[plane, 0, c, u, y * 16 : y * 16 + 16, lanes] = tile

        unpack(raw_in.at[way], v_recv.at[way], put)

    def unpack_left(p):
        def put(c, u, y, lanes, tile):
            left[c, u, p * 32 + y * 16 : p * 32 + y * 16 + 16, lanes] = tile

        unpack(rbuf.at[1, p], x_recv.at[1, p], put)

    def ring_copy(way, step, p):
        held = (z + 8 - step + 1) % 8 if way == 0 else (z + step - 1) % 8
        to = up if way == 0 else down
        if step < 4:
            piece = ring.at[held, p]
            return remote(
                piece, piece, r_send.at[way, step - 1, p], r_recv.at[way, step - 1, p], to, x, d
            )
        piece = ring.at[held, p, pl.ds(way * 2, 2)]
        return remote(piece, piece, h_send.at[way, p], h_recv.at[way, p], to, x, d)

    lane_group = lax.broadcasted_iota(jnp.int32, (96, 128), 1) // 32

    def multiply(plane, p):
        tile = None
        for c in range(4):
            total = None
            for u in range(2):
                rows = ring[plane, p, c, u]
                term = lax.dot_general(
                    left[c, u],
                    jnp.concatenate([rows] * 4, axis=0),
                    NT,
                    preferred_element_type=F32,
                )
                total = term if total is None else total + term
            tile = total if tile is None else jnp.where(lane_group == c, total, tile)
        tile = tile.astype(BF16)
        for ph in range(2):
            tsend[(plane * 3 + p) * 2 + ph] = jnp.concatenate(
                [tile[k * 32 + ph * 16 : k * 32 + ph * 16 + 16] for k in range(3)], axis=0
            )
        hand_out(plane, p)

    def hand_out(plane, p):
        pcol = plane // 2
        pcore = plane % 2
        slot = d * 8 + me
        for ph in range(2):
            for rel in range(2):
                prow = z * 2 + ph
                pd = ((yl + rel) % 2) * 2 + pcore
                unit = tsend.at[(plane * 3 + p) * 2 + ph]
                copy = remote(
                    unit, trecv.at[p, slot], t_send.at[rel], t_recv.at[p], prow, pcol, pd
                )
                if rel == 1:
                    copy.start()
                    continue
                other = jnp.logical_or(prow != row, jnp.logical_or(pcol != x, pd != d))

                @pl.when(other)
                def _():
                    copy.start()

                @pl.when(jnp.logical_not(other))
                def _():
                    pltpu.make_async_copy(unit, trecv.at[p, slot], t_recv.at[p]).start()

    def start_ring(p):
        ring_copy(0, 1, p).start()
        ring_copy(1, 1, p).start()

    project(0)
    pack(0, 0)
    project(1)
    pack(0, 1)
    pl.semaphore_wait(barrier, 33)
    raw_copy(0).start()
    raw_copy(1).start()
    exchange(0, 1)
    project(2)
    pack(0, 2)
    exchange(0, 2)
    for p in range(3):
        pack(1, p)
    unpack_right(1)
    start_ring(1)
    raw_spread(0)
    raw_spread(1)
    unpack_right(2)
    start_ring(2)
    exchange(0, 0)
    for p in range(3):
        exchange(1, p)

    mine = pl.ds(pl.multiple_of(core * 96, 96), 96)

    def gate_rows(n, carry):
        at = pl.ds(n * 4, 4)
        logits = (
            jnp.dot(
                normed[at, mine, :].reshape(384, 128),
                gate_weight[...],
                preferred_element_type=F32,
            )
            + gate_bias[...]
        )
        gate[at] = jax.nn.sigmoid(logits).reshape(4, 96, 128)
        return carry

    lax.fori_loop(0, 12, gate_rows, 0)
    table[0] = jnp.broadcast_to(out_gain[...], (128, 128)).T
    table[1] = jnp.broadcast_to(out_shift[...], (128, 128)).T
    table[2] = out_weight[...].astype(F32)

    for step in range(1, 5):
        plus = (z + 8 - step) % 8
        minus = (z + step) % 8
        for p in ORDER:
            for way in range(2):
                if step == 1 and p == 0:
                    unpack_raw(way)
                else:
                    ring_copy(way, step, p).wait_recv()
                if step < 4:
                    ring_copy(way, step + 1, p).start()
            if step > 1:
                multiply(plus, p)
                if step < 4:
                    multiply(minus, p)
        if step == 1:
            unpack_right(0)
            for p in range(3):
                unpack_left(p)
            for p in range(3):
                multiply(z, p)
                multiply(plus, p)
                multiply(minus, p)

    def regroup(n):
        return jnp.concatenate(
            [table[n, pl.ds(c, 32, stride=4), :] for c in range(4)], axis=0
        )

    gains = regroup(0)
    shifts = regroup(1)
    weight = regroup(2).astype(BF16)
    group = lax.broadcasted_iota(jnp.int32, (32, 128), 1) // 32

    def swap(p, k):
        part = out.at[:, pl.ds(pl.multiple_of(core * 96 + k * 24 + p * 8, 8), 8), :]
        return remote(
            part, part, o_send.at[p, k], o_recv.at[p, k], row, x, yl * 2 + 1 - core
        )

    def drain():
        for kind in range(2):
            for p in range(3):
                pltpu.make_async_copy(
                    sbuf.at[kind, p, pl.ds(0, 7)], rbuf.at[kind, p, pl.ds(0, 7)], x_send.at[kind, p]
                ).wait()
        for way in range(2):
            raw_copy(way).wait_send()
            pltpu.make_async_copy(
                raw.at[way, pl.ds(0, 7)], raw_in.at[way, pl.ds(0, 7)], v_send.at[way]
            ).wait()
        for step in range(1, 5):
            for p in range(3):
                for way in range(2):
                    if step > 1 or p > 0:
                        ring_copy(way, step, p).wait_send()
        for rel in range(2):
            units = tsend.at[pl.ds(0, 45 if rel == 0 else 48)]
            pltpu.make_async_copy(units, units, t_send.at[rel]).wait()

    for p in ORDER:
        if p == ORDER[2]:
            drain()
        pltpu.make_async_copy(trecv.at[p], trecv.at[p], t_recv.at[p]).wait()

        def widen(s, carry, p=p):
            at = pl.ds(pl.multiple_of(s * 192, 192), 192)
            wide[at, :] = trecv[p, pl.ds(s * 4, 4)].reshape(192, 128).astype(F32)
            return carry

        lax.fori_loop(0, 8, widen, 0, unroll=2)

        def finish(g, carry, p=p):
            from_row = [wide[pl.ds(g * 4 + i, 32, stride=48), :] for i in range(4)]
            blocks = []
            for c in range(4):
                block = None
                for i in range(4):
                    turn = (32 * (i - c)) % 128
                    moved = pltpu.roll(from_row[i], turn, 1) if turn else from_row[i]
                    block = moved if block is None else jnp.where(group == i, moved, block)
                blocks.append(block)
            vals = jnp.concatenate(blocks, axis=0)
            centred = vals - jnp.mean(vals, axis=0, keepdims=True)
            spread = jnp.mean(centred * centred, axis=0, keepdims=True)
            rows = (centred * lax.rsqrt(spread + EPS) * gains + shifts).astype(BF16)
            normal[pl.ds(pl.multiple_of(g * 128, 128), 128), :] = rows.T
            return carry

        lax.fori_loop(0, 12, finish, 0, unroll=UNROLL)

        def apply(g, carry, p=p):
            rows = normal[pl.ds(pl.multiple_of(g * 256, 256), 256), :]
            projected = jnp.dot(rows, weight, preferred_element_type=F32) + out_bias[...]
            for i in range(8):
                line = (g % 2) * 24 + (g // 2) * 8 + i
                for k in range(4):
                    j = k * 24 + p * 8
                    value = (
                        gate[line, j : j + 8, :]
                        * projected[i * 32 + k * 8 : i * 32 + k * 8 + 8]
                    )
                    out[line, pl.ds(pl.multiple_of(core * 96 + j, 8), 8), :] = value.astype(BF16)
            return carry

        lax.fori_loop(0, 6, apply, 0, unroll=2)
        for k in range(4):
            swap(p, k).start()

    for p in range(3):
        for k in range(4):
            swap(p, k).wait()


def per_device(
    pair,
    ln_gain,
    ln_shift,
    proj_weight,
    proj_bias,
    gate_weight,
    gate_bias,
    out_gain,
    out_shift,
    out_weight,
    out_bias,
):
    line = lambda v: v.reshape(1, -1)
    operands = (
        pair,
        line(ln_gain),
        line(ln_shift),
        proj_weight,
        line(proj_bias),
        gate_weight,
        line(gate_bias),
        line(out_gain),
        line(out_shift),
        out_weight,
        line(out_bias),
    )
    vmem = pl.BlockSpec(memory_space=pltpu.VMEM)
    dma = pltpu.SemaphoreType.DMA
    return pl.pallas_call(
        kernel,
        out_shape=jax.ShapeDtypeStruct(pair.shape, BF16),
        in_specs=[pl.BlockSpec(memory_space=pl.ANY)] * 11,
        out_specs=vmem,
        scratch_shapes=[
            *[pltpu.VMEM(v.shape, v.dtype) for v in operands[1:]],
            pltpu.VMEM((48, 192, 128), BF16),
            pltpu.VMEM((512, 128), BF16),
            pltpu.VMEM((512, 128), F32),
            pltpu.VMEM((48, 192, 128), BF16),
            pltpu.VMEM((48, 96, 128), F32),
            pltpu.VMEM((2, 3, 3, 256, 128), F32),
            pltpu.VMEM((2, 3, 8, 32, 384), BF16),
            pltpu.VMEM((2, 3, 8, 32, 384), BF16),
            pltpu.VMEM((4, 2, 96, 384), BF16),
            pltpu.VMEM((8, 3, 4, 2, 32, 384), BF16),
            pltpu.VMEM((48, 48, 128), BF16),
            pltpu.VMEM((3, 32, 48, 128), BF16),
            pltpu.VMEM((1536, 128), F32),
            pltpu.VMEM((3, 128, 128), F32),
            pltpu.VMEM((1536, 128), BF16),
            pltpu.VMEM((2, 8, 32, 384), BF16),
            pltpu.VMEM((2, 8, 32, 384), BF16),
            dma((10,)),
            dma((3, 2)),
            dma((2,)),
            dma((2,)),
            dma((2,)),
            dma((2,)),
            dma((2, 3)),
            dma((2, 3)),
            dma((2, 3, 3)),
            dma((2, 3, 3)),
            dma((2, 3)),
            dma((2, 3)),
            dma((2,)),
            dma((3,)),
            dma((3, 4)),
            dma((3, 4)),
        ],
        compiler_params=pltpu.CompilerParams(
            collective_id=0, has_side_effects=True, vmem_limit_bytes=VMEM_MIB * 1024 * 1024
        ),
    )(*[pltpu.with_memory_space_constraint(v, pltpu.HBM) for v in operands])


def solution(mesh):
    in_specs = (P("row", "col", None),) + (P(),) * 10
    return jax.shard_map(
        per_device, mesh=mesh, in_specs=in_specs, out_specs=P("row", "col", None), check_vma=False
    )
```

```python
import functools

import jax
import jax.numpy as jnp
from jax import lax
from jax.experimental import pallas as pl
from jax.experimental.pallas import tpu as pltpu
from jax.sharding import PartitionSpec as P

F32 = jnp.float32
BF16 = jnp.bfloat16
EPS = 1e-05
NT = (((1,), (1,)), ((), ()))
VMEM_MIB = 50
UNROLL = 6
ORDER = (1, 2, 0)


def remote(src, dst, send_sem, recv_sem, row, col, depth):
    return pltpu.make_async_remote_copy(
        src_ref=src,
        dst_ref=dst,
        send_sem=send_sem,
        recv_sem=recv_sem,
        device_id=(row, col, depth),
        device_id_type=pl.DeviceIdType.MESH,
    )


def kernel(*refs):
    work(refs[0], refs[1:11], refs[12:22], refs[11], *refs[12:])


def work(
    pair_hbm,
    sources,
    params,
    out,
    ln_gain,
    ln_shift,
    proj_weight,
    proj_bias,
    gate_weight,
    gate_bias,
    out_gain,
    out_shift,
    out_weight,
    out_bias,
    pair,
    wt,
    bt,
    normed,
    gate,
    stage,
    sbuf,
    rbuf,
    left,
    ring,
    tsend,
    trecv,
    wide,
    table,
    normal,
    raw,
    raw_in,
    w_sem,
    p_sem,
    w_send,
    w_recv,
    v_send,
    v_recv,
    x_send,
    x_recv,
    r_send,
    r_recv,
    h_send,
    h_recv,
    t_send,
    t_recv,
    o_send,
    o_recv,
):
    row = lax.axis_index("row")
    x = lax.axis_index("col")
    d = lax.axis_index("depth")
    z = row // 2
    yh = row % 2
    yl = d // 2
    core = d % 2
    me = x * 2 + yh

    def load(p, half):
        rows = pl.ds(half * 24 + p * 8, 8)
        return pltpu.make_async_copy(pair_hbm.at[rows], pair.at[rows], p_sem.at[p, half])

    for half in range(2):
        load(0, half).start()
    fetches = [
        pltpu.make_async_copy(src, dst, w_sem.at[n])
        for n, (src, dst) in enumerate(zip(sources, params))
    ]
    for fetch in fetches:
        fetch.start()
    for p in range(1, 3):
        for half in range(2):
            load(p, half).start()

    barrier = pltpu.get_barrier_semaphore()

    up = (row + 2) % 16
    down = (row + 14) % 16
    greeted = [
        (z * 2 + (yh + a) % 2, (x + b) % 4, (d + e) % 4)
        for b in (2, 1, 3, 0)
        for a in (1, 0)
        for e in (2, 1, 3, 0)
        if a or b or e
    ]
    for device in greeted + [(up, x, d), (down, x, d)]:
        pl.semaphore_signal(
            barrier, inc=1, device_id=device, device_id_type=pl.DeviceIdType.MESH
        )

    for fetch in fetches:
        fetch.wait()

    for b in range(4):
        wt[b * 128 : (b + 1) * 128, :] = (
            proj_weight[:, b * 128 : (b + 1) * 128].astype(F32).T.astype(BF16)
        )
        bt[b * 128 : (b + 1) * 128, :] = jnp.broadcast_to(
            proj_bias[:, b * 128 : (b + 1) * 128], (128, 128)
        ).T
    first = pl.multiple_of(d * 32, 32)
    wsel = jnp.concatenate([wt[pl.ds(first + 128 * b, 32), :] for b in range(4)], axis=0)
    gain = ln_gain[...]
    shift = ln_shift[...]

    def project(p):
        def body(n, carry):
            t = p * 8 + n
            vals = jnp.concatenate([pair[t], pair[t + 24]], axis=0).astype(F32)
            centred = vals - jnp.mean(vals, axis=-1, keepdims=True)
            spread = jnp.mean(centred * centred, axis=-1, keepdims=True)
            rows = (centred * lax.rsqrt(spread + EPS) * gain + shift).astype(BF16)
            normed[t] = rows[:192]
            normed[t + 24] = rows[192:]
            mixed = lax.dot_general(wsel, rows, NT, preferred_element_type=F32)
            at = pl.ds(pl.multiple_of(n * 32, 32), 32)
            for q in range(3):
                cut = [
                    mixed[b * 32 : (b + 1) * 32, q * 128 : (q + 1) * 128]
                    + bt[pl.ds(first + 128 * b, 32), :]
                    for b in range(4)
                ]
                stage[0, p, q, at, :] = jax.nn.sigmoid(cut[2]) * cut[3]
                stage[1, p, q, at, :] = jax.nn.sigmoid(cut[0]) * cut[1]
            return carry

        for half in range(2):
            load(p, half).wait()
        lax.fori_loop(0, 8, body, 0, unroll=2)

    def pack(kind, p):
        def body(g, carry):
            for q in range(3):
                rows = [
                    stage[kind, p, q, pl.ds(g * 4 + c, 8, stride=32), :] for c in range(4)
                ]
                sbuf[kind, p, g, :, q * 128 : (q + 1) * 128] = jnp.concatenate(
                    rows, axis=0
                ).astype(BF16)
            return carry

        lax.fori_loop(0, 8, body, 0, unroll=2)

    def spread(source, target, send_sem, recv_sem):
        for n in (5, 4, 3, 1, 2, 6, 7):
            g = (me + n) % 8
            remote(
                source.at[g], target.at[me], send_sem, recv_sem, z * 2 + g % 2, g // 2, d
            ).start()
        pltpu.make_async_copy(source.at[me], target.at[me], recv_sem).start()

    def exchange(kind, p):
        spread(sbuf.at[kind, p], rbuf.at[kind, p], x_send.at[kind, p], x_recv.at[kind, p])

    def raw_copy(way):
        to = up if way == 0 else down
        return remote(sbuf.at[0, 0], raw.at[way], w_send.at[way], w_recv.at[way], to, x, d)

    def raw_spread(way):
        raw_copy(way).wait_recv()
        spread(raw.at[way], raw_in.at[way], v_send.at[way], v_recv.at[way])

    low = lax.broadcasted_iota(jnp.int32, (32, 128), 1) < 64

    def unpack(source, recv_sem, put):
        pltpu.make_async_copy(source, source, recv_sem).wait()
        for u in range(2):
            for y in range(2):
                one = source[4 * u + y].astype(F32)
                two = source[4 * u + 2 + y].astype(F32)
                a = [one[:, q * 128 : (q + 1) * 128] for q in range(3)]
                b = [two[:, q * 128 : (q + 1) * 128] for q in range(3)]
                ra1 = pltpu.roll(a[1], 64, 1)
                ra2 = pltpu.roll(a[2], 64, 1)
                rb0 = pltpu.roll(b[0], 64, 1)
                rb1 = pltpu.roll(b[1], 64, 1)
                evens = [a[0], jnp.where(low, a[1], rb0), jnp.where(low, rb0, rb1)]
                odds = [jnp.where(low, ra1, ra2), jnp.where(low, ra2, b[1]), b[2]]
                for c in range(4):
                    at = slice(c * 8, c * 8 + 8)
                    for q in range(3):
                        put(
                            c, u, y, slice(q * 128, q * 128 + 128),
                            jnp.concatenate([evens[q][at], odds[q][at]], axis=0).astype(BF16),
                        )

    def unpack_right(p):
        def put(c, u, y, lanes, tile):
            ring[z, p, c, u, y * 16 : y * 16 + 16, lanes] = tile

        unpack(rbuf.at[0, p], x_recv.at[0, p], put)

    def unpack_raw(way):
        plane = (z + 7) % 8 if way == 0 else (z + 1) % 8

        def put(c, u, y, lanes, tile):
            ring[plane, 0, c, u, y * 16 : y * 16 + 16, lanes] = tile

        unpack(raw_in.at[way], v_recv.at[way], put)

    def unpack_left(p):
        def put(c, u, y, lanes, tile):
            left[c, u, p * 32 + y * 16 : p * 32 + y * 16 + 16, lanes] = tile

        unpack(rbuf.at[1, p], x_recv.at[1, p], put)

    def ring_copy(way, step, p):
        held = (z + 8 - step + 1) % 8 if way == 0 else (z + step - 1) % 8
        to = up if way == 0 else down
        if step < 4:
            piece = ring.at[held, p]
            return remote(
                piece, piece, r_send.at[way, step - 1, p], r_recv.at[way, step - 1, p], to, x, d
            )
        piece = ring.at[held, p, pl.ds(way * 2, 2)]
        return remote(piece, piece, h_send.at[way, p], h_recv.at[way, p], to, x, d)

    lane_group = lax.broadcasted_iota(jnp.int32, (96, 128), 1) // 32

    def multiply(plane, p):
        tile = None
        for c in range(4):
            total = None
            for u in range(2):
                rows = ring[plane, p, c, u]
                term = lax.dot_general(
                    left[c, u],
                    jnp.concatenate([rows] * 4, axis=0),
                    NT,
                    preferred_element_type=F32,
                )
                total = term if total is None else total + term
            tile = total if tile is None else jnp.where(lane_group == c, total, tile)
        tile = tile.astype(BF16)
        for ph in range(2):
            tsend[(plane * 3 + p) * 2 + ph] = jnp.concatenate(
                [tile[k * 32 + ph * 16 : k * 32 + ph * 16 + 16] for k in range(3)], axis=0
            )
        hand_out(plane, p)

    def hand_out(plane, p):
        pcol = plane // 2
        pcore = plane % 2
        slot = d * 8 + me
        for ph in range(2):
            for rel in range(2):
                prow = z * 2 + ph
                pd = ((yl + rel) % 2) * 2 + pcore
                unit = tsend.at[(plane * 3 + p) * 2 + ph]
                copy = remote(
                    unit, trecv.at[p, slot], t_send.at[rel], t_recv.at[p], prow, pcol, pd
                )
                if rel == 1:
                    copy.start()
                    continue
                other = jnp.logical_or(prow != row, jnp.logical_or(pcol != x, pd != d))

                @pl.when(other)
                def _():
                    copy.start()

                @pl.when(jnp.logical_not(other))
                def _():
                    pltpu.make_async_copy(unit, trecv.at[p, slot], t_recv.at[p]).start()

    def start_ring(p):
        ring_copy(0, 1, p).start()
        ring_copy(1, 1, p).start()

    project(0)
    pack(0, 0)
    project(1)
    pack(0, 1)
    pl.semaphore_wait(barrier, 33)
    raw_copy(0).start()
    raw_copy(1).start()
    exchange(0, 1)
    project(2)
    pack(0, 2)
    exchange(0, 2)
    pack(1, 0)
    exchange(1, 0)
    pack(1, 1)
    exchange(1, 1)
    pack(1, 2)
    unpack_right(1)
    start_ring(1)
    raw_spread(0)
    raw_spread(1)
    unpack_right(2)
    start_ring(2)
    exchange(1, 2)
    exchange(0, 0)

    mine = pl.ds(pl.multiple_of(core * 96, 96), 96)

    def gate_rows(n, carry):
        at = pl.ds(n * 4, 4)
        logits = (
            jnp.dot(
                normed[at, mine, :].reshape(384, 128),
                gate_weight[...],
                preferred_element_type=F32,
            )
            + gate_bias[...]
        )
        gate[at] = jax.nn.sigmoid(logits).reshape(4, 96, 128)
        return carry

    lax.fori_loop(0, 12, gate_rows, 0)
    table[0] = jnp.broadcast_to(out_gain[...], (128, 128)).T
    table[1] = jnp.broadcast_to(out_shift[...], (128, 128)).T
    table[2] = out_weight[...].astype(F32)

    def forward(step, p):
        for way in range(2):
            if step == 1 and p == 0:
                unpack_raw(way)
            else:
                ring_copy(way, step, p).wait_recv()
            if step < 4:
                ring_copy(way, step + 1, p).start()

    def multiply_both(step, p):
        multiply((z + 8 - step) % 8, p)
        multiply((z + step) % 8, p)

    for p in ORDER:
        forward(1, p)
    forward(2, 1)
    forward(2, 2)
    for p in range(3):
        unpack_left(p)
    unpack_right(0)
    forward(2, 0)
    for p in range(3):
        multiply(z, p)
        multiply_both(1, p)
    forward(3, 1)
    multiply_both(2, 1)
    multiply_both(2, 2)
    forward(3, 2)
    multiply_both(2, 0)
    multiply_both(3, 1)
    forward(3, 0)
    multiply_both(3, 2)
    multiply_both(3, 0)
    for p in ORDER:
        forward(4, p)
        multiply((z + 4) % 8, p)

    def regroup(n):
        return jnp.concatenate(
            [table[n, pl.ds(c, 32, stride=4), :] for c in range(4)], axis=0
        )

    gains = regroup(0)
    shifts = regroup(1)
    weight = regroup(2).astype(BF16)
    group = lax.broadcasted_iota(jnp.int32, (32, 128), 1) // 32

    def swap(p, k):
        part = out.at[:, pl.ds(pl.multiple_of(core * 96 + k * 24 + p * 8, 8), 8), :]
        return remote(
            part, part, o_send.at[p, k], o_recv.at[p, k], row, x, yl * 2 + 1 - core
        )

    def drain():
        for kind in range(2):
            for p in range(3):
                pltpu.make_async_copy(
                    sbuf.at[kind, p, pl.ds(0, 7)], rbuf.at[kind, p, pl.ds(0, 7)], x_send.at[kind, p]
                ).wait()
        for way in range(2):
            raw_copy(way).wait_send()
            pltpu.make_async_copy(
                raw.at[way, pl.ds(0, 7)], raw_in.at[way, pl.ds(0, 7)], v_send.at[way]
            ).wait()
        for step in range(1, 5):
            for p in range(3):
                for way in range(2):
                    if step > 1 or p > 0:
                        ring_copy(way, step, p).wait_send()
        for rel in range(2):
            units = tsend.at[pl.ds(0, 45 if rel == 0 else 48)]
            pltpu.make_async_copy(units, units, t_send.at[rel]).wait()

    for p in ORDER:
        if p == ORDER[2]:
            drain()
        pltpu.make_async_copy(trecv.at[p], trecv.at[p], t_recv.at[p]).wait()

        def widen(s, carry, p=p):
            at = pl.ds(pl.multiple_of(s * 192, 192), 192)
            wide[at, :] = trecv[p, pl.ds(s * 4, 4)].reshape(192, 128).astype(F32)
            return carry

        lax.fori_loop(0, 8, widen, 0, unroll=2)

        def finish(g, carry, p=p):
            from_row = [wide[pl.ds(g * 4 + i, 32, stride=48), :] for i in range(4)]
            blocks = []
            for c in range(4):
                block = None
                for i in range(4):
                    turn = (32 * (i - c)) % 128
                    moved = pltpu.roll(from_row[i], turn, 1) if turn else from_row[i]
                    block = moved if block is None else jnp.where(group == i, moved, block)
                blocks.append(block)
            vals = jnp.concatenate(blocks, axis=0)
            centred = vals - jnp.mean(vals, axis=0, keepdims=True)
            spread = jnp.mean(centred * centred, axis=0, keepdims=True)
            rows = (centred * lax.rsqrt(spread + EPS) * gains + shifts).astype(BF16)
            normal[pl.ds(pl.multiple_of(g * 128, 128), 128), :] = rows.T
            return carry

        lax.fori_loop(0, 12, finish, 0, unroll=UNROLL)

        def apply(g, carry, p=p):
            rows = normal[pl.ds(pl.multiple_of(g * 256, 256), 256), :]
            projected = jnp.dot(rows, weight, preferred_element_type=F32) + out_bias[...]
            for i in range(8):
                line = (g % 2) * 24 + (g // 2) * 8 + i
                for k in range(4):
                    j = k * 24 + p * 8
                    value = (
                        gate[line, j : j + 8, :]
                        * projected[i * 32 + k * 8 : i * 32 + k * 8 + 8]
                    )
                    out[line, pl.ds(pl.multiple_of(core * 96 + j, 8), 8), :] = value.astype(BF16)
            return carry

        lax.fori_loop(0, 6, apply, 0, unroll=2)
        for k in range(4):
            swap(p, k).start()

    for p in range(3):
        for k in range(4):
            swap(p, k).wait()


def per_device(
    pair,
    ln_gain,
    ln_shift,
    proj_weight,
    proj_bias,
    gate_weight,
    gate_bias,
    out_gain,
    out_shift,
    out_weight,
    out_bias,
):
    line = lambda v: v.reshape(1, -1)
    operands = (
        pair,
        line(ln_gain),
        line(ln_shift),
        proj_weight,
        line(proj_bias),
        gate_weight,
        line(gate_bias),
        line(out_gain),
        line(out_shift),
        out_weight,
        line(out_bias),
    )
    vmem = pl.BlockSpec(memory_space=pltpu.VMEM)
    dma = pltpu.SemaphoreType.DMA
    return pl.pallas_call(
        kernel,
        out_shape=jax.ShapeDtypeStruct(pair.shape, BF16),
        in_specs=[pl.BlockSpec(memory_space=pl.ANY)] * 11,
        out_specs=vmem,
        scratch_shapes=[
            *[pltpu.VMEM(v.shape, v.dtype) for v in operands[1:]],
            pltpu.VMEM((48, 192, 128), BF16),
            pltpu.VMEM((512, 128), BF16),
            pltpu.VMEM((512, 128), F32),
            pltpu.VMEM((48, 192, 128), BF16),
            pltpu.VMEM((48, 96, 128), F32),
            pltpu.VMEM((2, 3, 3, 256, 128), F32),
            pltpu.VMEM((2, 3, 8, 32, 384), BF16),
            pltpu.VMEM((2, 3, 8, 32, 384), BF16),
            pltpu.VMEM((4, 2, 96, 384), BF16),
            pltpu.VMEM((8, 3, 4, 2, 32, 384), BF16),
            pltpu.VMEM((48, 48, 128), BF16),
            pltpu.VMEM((3, 32, 48, 128), BF16),
            pltpu.VMEM((1536, 128), F32),
            pltpu.VMEM((3, 128, 128), F32),
            pltpu.VMEM((1536, 128), BF16),
            pltpu.VMEM((2, 8, 32, 384), BF16),
            pltpu.VMEM((2, 8, 32, 384), BF16),
            dma((10,)),
            dma((3, 2)),
            dma((2,)),
            dma((2,)),
            dma((2,)),
            dma((2,)),
            dma((2, 3)),
            dma((2, 3)),
            dma((2, 3, 3)),
            dma((2, 3, 3)),
            dma((2, 3)),
            dma((2, 3)),
            dma((2,)),
            dma((3,)),
            dma((3, 4)),
            dma((3, 4)),
        ],
        compiler_params=pltpu.CompilerParams(
            collective_id=0, has_side_effects=True, vmem_limit_bytes=VMEM_MIB * 1024 * 1024
        ),
    )(*[pltpu.with_memory_space_constraint(v, pltpu.HBM) for v in operands])


def solution(mesh):
    in_specs = (P("row", "col", None),) + (P(),) * 10
    return jax.shard_map(
        per_device, mesh=mesh, in_specs=in_specs, out_specs=P("row", "col", None), check_vma=False
    )
```

```python
import functools

import jax
import jax.numpy as jnp
from jax import lax
from jax.experimental import pallas as pl
from jax.experimental.pallas import tpu as pltpu
from jax.sharding import PartitionSpec as P

F32 = jnp.float32
BF16 = jnp.bfloat16
EPS = 1e-05
NT = (((1,), (1,)), ((), ()))
VMEM_MIB = 50
UNROLL = 6
ORDER = (1, 2, 0)


def remote(src, dst, send_sem, recv_sem, row, col, depth):
    return pltpu.make_async_remote_copy(
        src_ref=src,
        dst_ref=dst,
        send_sem=send_sem,
        recv_sem=recv_sem,
        device_id=(row, col, depth),
        device_id_type=pl.DeviceIdType.MESH,
    )


def kernel(*refs):
    work(refs[0], refs[1:11], refs[12:22], refs[11], *refs[12:])


def work(
    pair_hbm,
    sources,
    params,
    out,
    ln_gain,
    ln_shift,
    proj_weight,
    proj_bias,
    gate_weight,
    gate_bias,
    out_gain,
    out_shift,
    out_weight,
    out_bias,
    pair,
    wt,
    bt,
    normed,
    gate,
    stage,
    sbuf,
    rbuf,
    left,
    ring,
    tsend,
    trecv,
    wide,
    table,
    normal,
    raw,
    raw_in,
    w_sem,
    p_sem,
    w_send,
    w_recv,
    v_send,
    v_recv,
    x_send,
    x_recv,
    r_send,
    r_recv,
    h_send,
    h_recv,
    t_send,
    t_recv,
    o_send,
    o_recv,
):
    row = lax.axis_index("row")
    x = lax.axis_index("col")
    d = lax.axis_index("depth")
    z = row // 2
    yh = row % 2
    yl = d // 2
    core = d % 2
    me = x * 2 + yh

    def load(p, half):
        rows = pl.ds(half * 24 + p * 8, 8)
        return pltpu.make_async_copy(pair_hbm.at[rows], pair.at[rows], p_sem.at[p, half])

    for half in range(2):
        load(0, half).start()
    fetches = [
        pltpu.make_async_copy(src, dst, w_sem.at[n])
        for n, (src, dst) in enumerate(zip(sources, params))
    ]
    for fetch in fetches:
        fetch.start()
    for p in range(1, 3):
        for half in range(2):
            load(p, half).start()

    barrier = pltpu.get_barrier_semaphore()

    up = (row + 2) % 16
    down = (row + 14) % 16
    greeted = [
        (z * 2 + (yh + a) % 2, (x + b) % 4, (d + e) % 4)
        for b in (2, 1, 3, 0)
        for a in (1, 0)
        for e in (2, 1, 3, 0)
        if a or b or e
    ]
    for device in greeted + [(up, x, d), (down, x, d)]:
        pl.semaphore_signal(
            barrier, inc=1, device_id=device, device_id_type=pl.DeviceIdType.MESH
        )

    for fetch in fetches:
        fetch.wait()

    for b in range(4):
        wt[b * 128 : (b + 1) * 128, :] = (
            proj_weight[:, b * 128 : (b + 1) * 128].astype(F32).T.astype(BF16)
        )
        bt[b * 128 : (b + 1) * 128, :] = jnp.broadcast_to(
            proj_bias[:, b * 128 : (b + 1) * 128], (128, 128)
        ).T
    first = pl.multiple_of(d * 32, 32)
    wsel = jnp.concatenate([wt[pl.ds(first + 128 * b, 32), :] for b in range(4)], axis=0)
    gain = ln_gain[...]
    shift = ln_shift[...]

    def project(p):
        def body(n, carry):
            t = p * 8 + n
            vals = jnp.concatenate([pair[t], pair[t + 24]], axis=0).astype(F32)
            centred = vals - jnp.mean(vals, axis=-1, keepdims=True)
            spread = jnp.mean(centred * centred, axis=-1, keepdims=True)
            rows = (centred * lax.rsqrt(spread + EPS) * gain + shift).astype(BF16)
            normed[t] = rows[:192]
            normed[t + 24] = rows[192:]
            mixed = lax.dot_general(wsel, rows, NT, preferred_element_type=F32)
            at = pl.ds(pl.multiple_of(n * 32, 32), 32)
            for q in range(3):
                cut = [
                    mixed[b * 32 : (b + 1) * 32, q * 128 : (q + 1) * 128]
                    + bt[pl.ds(first + 128 * b, 32), :]
                    for b in range(4)
                ]
                stage[0, p, q, at, :] = jax.nn.sigmoid(cut[2]) * cut[3]
                stage[1, p, q, at, :] = jax.nn.sigmoid(cut[0]) * cut[1]
            return carry

        for half in range(2):
            load(p, half).wait()
        lax.fori_loop(0, 8, body, 0, unroll=2)

    def pack(kind, p):
        def body(g, carry):
            for q in range(3):
                rows = [
                    stage[kind, p, q, pl.ds(g * 4 + c, 8, stride=32), :] for c in range(4)
                ]
                sbuf[kind, p, g, :, q * 128 : (q + 1) * 128] = jnp.concatenate(
                    rows, axis=0
                ).astype(BF16)
            return carry

        lax.fori_loop(0, 8, body, 0, unroll=2)

    def spread(source, target, send_sem, recv_sem):
        for n in (5, 4, 3, 1, 2, 6, 7):
            g = (me + n) % 8
            remote(
                source.at[g], target.at[me], send_sem, recv_sem, z * 2 + g % 2, g // 2, d
            ).start()
        pltpu.make_async_copy(source.at[me], target.at[me], recv_sem).start()

    def exchange(kind, p):
        spread(sbuf.at[kind, p], rbuf.at[kind, p], x_send.at[kind, p], x_recv.at[kind, p])

    def raw_copy(way):
        to = up if way == 0 else down
        return remote(sbuf.at[0, 0], raw.at[way], w_send.at[way], w_recv.at[way], to, x, d)

    def raw_spread(way):
        raw_copy(way).wait_recv()
        spread(raw.at[way], raw_in.at[way], v_send.at[way], v_recv.at[way])

    low = lax.broadcasted_iota(jnp.int32, (32, 128), 1) < 64

    def unpack(source, recv_sem, put):
        pltpu.make_async_copy(source, source, recv_sem).wait()
        for u in range(2):
            for y in range(2):
                one = source[4 * u + y].astype(F32)
                two = source[4 * u + 2 + y].astype(F32)
                a = [one[:, q * 128 : (q + 1) * 128] for q in range(3)]
                b = [two[:, q * 128 : (q + 1) * 128] for q in range(3)]
                ra1 = pltpu.roll(a[1], 64, 1)
                ra2 = pltpu.roll(a[2], 64, 1)
                rb0 = pltpu.roll(b[0], 64, 1)
                rb1 = pltpu.roll(b[1], 64, 1)
                evens = [a[0], jnp.where(low, a[1], rb0), jnp.where(low, rb0, rb1)]
                odds = [jnp.where(low, ra1, ra2), jnp.where(low, ra2, b[1]), b[2]]
                for c in range(4):
                    at = slice(c * 8, c * 8 + 8)
                    for q in range(3):
                        put(
                            c, u, y, slice(q * 128, q * 128 + 128),
                            jnp.concatenate([evens[q][at], odds[q][at]], axis=0).astype(BF16),
                        )

    def unpack_right(p):
        def put(c, u, y, lanes, tile):
            ring[z, p, c, u, y * 16 : y * 16 + 16, lanes] = tile

        unpack(rbuf.at[0, p], x_recv.at[0, p], put)

    def unpack_raw(way):
        plane = (z + 7) % 8 if way == 0 else (z + 1) % 8

        def put(c, u, y, lanes, tile):
            ring[plane, 0, c, u, y * 16 : y * 16 + 16, lanes] = tile

        unpack(raw_in.at[way], v_recv.at[way], put)

    def unpack_left(p):
        def put(c, u, y, lanes, tile):
            left[c, u, p * 32 + y * 16 : p * 32 + y * 16 + 16, lanes] = tile

        unpack(rbuf.at[1, p], x_recv.at[1, p], put)

    def ring_copy(way, step, p):
        held = (z + 8 - step + 1) % 8 if way == 0 else (z + step - 1) % 8
        to = up if way == 0 else down
        if step < 4:
            piece = ring.at[held, p]
            return remote(
                piece, piece, r_send.at[way, step - 1, p], r_recv.at[way, step - 1, p], to, x, d
            )
        piece = ring.at[held, p, pl.ds(way * 2, 2)]
        return remote(piece, piece, h_send.at[way, p], h_recv.at[way, p], to, x, d)

    lane_group = lax.broadcasted_iota(jnp.int32, (96, 128), 1) // 32

    def multiply(plane, p):
        tile = None
        for c in range(4):
            total = None
            for u in range(2):
                rows = ring[plane, p, c, u]
                term = lax.dot_general(
                    left[c, u],
                    jnp.concatenate([rows] * 4, axis=0),
                    NT,
                    preferred_element_type=F32,
                )
                total = term if total is None else total + term
            tile = total if tile is None else jnp.where(lane_group == c, total, tile)
        tile = tile.astype(BF16)
        for ph in range(2):
            tsend[(plane * 3 + p) * 2 + ph] = jnp.concatenate(
                [tile[k * 32 + ph * 16 : k * 32 + ph * 16 + 16] for k in range(3)], axis=0
            )
        hand_out(plane, p)

    def hand_out(plane, p):
        pcol = plane // 2
        pcore = plane % 2
        slot = d * 8 + me
        for ph in range(2):
            for rel in range(2):
                prow = z * 2 + ph
                pd = ((yl + rel) % 2) * 2 + pcore
                unit = tsend.at[(plane * 3 + p) * 2 + ph]
                copy = remote(
                    unit, trecv.at[p, slot], t_send.at[rel], t_recv.at[p], prow, pcol, pd
                )
                if rel == 1:
                    copy.start()
                    continue
                other = jnp.logical_or(prow != row, jnp.logical_or(pcol != x, pd != d))

                @pl.when(other)
                def _():
                    copy.start()

                @pl.when(jnp.logical_not(other))
                def _():
                    pltpu.make_async_copy(unit, trecv.at[p, slot], t_recv.at[p]).start()

    def start_ring(p):
        ring_copy(0, 1, p).start()
        ring_copy(1, 1, p).start()

    project(0)
    pack(0, 0)
    project(1)
    pack(0, 1)
    pl.semaphore_wait(barrier, 33)
    raw_copy(0).start()
    raw_copy(1).start()
    exchange(0, 1)
    project(2)
    pack(0, 2)
    exchange(0, 2)
    for p in range(3):
        pack(1, p)
    unpack_right(1)
    start_ring(1)
    raw_spread(0)
    raw_spread(1)
    unpack_right(2)
    start_ring(2)
    exchange(0, 0)
    for p in range(3):
        exchange(1, p)

    mine = pl.ds(pl.multiple_of(core * 96, 96), 96)

    def gate_rows(n, carry):
        at = pl.ds(n * 4, 4)
        logits = (
            jnp.dot(
                normed[at, mine, :].reshape(384, 128),
                gate_weight[...],
                preferred_element_type=F32,
            )
            + gate_bias[...]
        )
        gate[at] = jax.nn.sigmoid(logits).reshape(4, 96, 128)
        return carry

    lax.fori_loop(0, 12, gate_rows, 0)
    table[0] = jnp.broadcast_to(out_gain[...], (128, 128)).T
    table[1] = jnp.broadcast_to(out_shift[...], (128, 128)).T
    table[2] = out_weight[...].astype(F32)

    for step in range(1, 5):
        plus = (z + 8 - step) % 8
        minus = (z + step) % 8
        for p in ORDER:
            for way in range(2):
                if step == 1 and p == 0:
                    unpack_raw(way)
                else:
                    ring_copy(way, step, p).wait_recv()
                if step < 4:
                    ring_copy(way, step + 1, p).start()
            if step > 1:
                multiply(plus, p)
                if step < 4:
                    multiply(minus, p)
        if step == 1:
            unpack_right(0)
            for p in range(3):
                unpack_left(p)
            for p in range(3):
                multiply(z, p)
                multiply(plus, p)
                multiply(minus, p)

    def regroup(n):
        return jnp.concatenate(
            [table[n, pl.ds(c, 32, stride=4), :] for c in range(4)], axis=0
        )

    gains = regroup(0)
    shifts = regroup(1)
    weight = regroup(2).astype(BF16)
    group = lax.broadcasted_iota(jnp.int32, (32, 128), 1) // 32

    def swap(p, half, k):
        columns = pl.ds(pl.multiple_of(core * 96 + k * 24 + p * 8, 8), 8)
        piece = out.at[pl.ds(half * 24, 24), columns, :]
        return remote(
            piece,
            piece,
            o_send.at[p, half, k],
            o_recv.at[p, half, k],
            row,
            x,
            yl * 2 + 1 - core,
        )

    def drain():
        for kind in range(2):
            for p in range(3):
                pltpu.make_async_copy(
                    sbuf.at[kind, p, pl.ds(0, 7)], rbuf.at[kind, p, pl.ds(0, 7)], x_send.at[kind, p]
                ).wait()
        for way in range(2):
            raw_copy(way).wait_send()
            pltpu.make_async_copy(
                raw.at[way, pl.ds(0, 7)], raw_in.at[way, pl.ds(0, 7)], v_send.at[way]
            ).wait()
        for step in range(1, 5):
            for p in range(3):
                for way in range(2):
                    if step > 1 or p > 0:
                        ring_copy(way, step, p).wait_send()
        for rel in range(2):
            units = tsend.at[pl.ds(0, 45 if rel == 0 else 48)]
            pltpu.make_async_copy(units, units, t_send.at[rel]).wait()

    for p in ORDER:
        if p == ORDER[2]:
            drain()
        pltpu.make_async_copy(trecv.at[p], trecv.at[p], t_recv.at[p]).wait()

        def widen(s, carry, p=p):
            at = pl.ds(pl.multiple_of(s * 192, 192), 192)
            wide[at, :] = trecv[p, pl.ds(s * 4, 4)].reshape(192, 128).astype(F32)
            return carry

        lax.fori_loop(0, 8, widen, 0, unroll=2)

        def finish(n, carry, half):
            g = (n // 2) * 4 + half * 2 + n % 2
            from_row = [wide[pl.ds(g * 4 + i, 32, stride=48), :] for i in range(4)]
            blocks = []
            for c in range(4):
                block = None
                for i in range(4):
                    turn = (32 * (i - c)) % 128
                    moved = pltpu.roll(from_row[i], turn, 1) if turn else from_row[i]
                    block = moved if block is None else jnp.where(group == i, moved, block)
                blocks.append(block)
            vals = jnp.concatenate(blocks, axis=0)
            centred = vals - jnp.mean(vals, axis=0, keepdims=True)
            spread = jnp.mean(centred * centred, axis=0, keepdims=True)
            rows = (centred * lax.rsqrt(spread + EPS) * gains + shifts).astype(BF16)
            at = pl.ds(pl.multiple_of(half * 768 + n * 128, 128), 128)
            normal[at, :] = rows.T
            return carry

        def apply(n, carry, half, p=p):
            rows = normal[pl.ds(pl.multiple_of(half * 768 + n * 256, 256), 256), :]
            projected = jnp.dot(rows, weight, preferred_element_type=F32) + out_bias[...]
            for i in range(8):
                line = half * 24 + n * 8 + i
                for k in range(4):
                    j = k * 24 + p * 8
                    value = (
                        gate[line, j : j + 8, :]
                        * projected[i * 32 + k * 8 : i * 32 + k * 8 + 8]
                    )
                    out[line, pl.ds(pl.multiple_of(core * 96 + j, 8), 8), :] = value.astype(BF16)
            return carry

        for half in range(2):
            lax.fori_loop(0, 6, functools.partial(finish, half=half), 0, unroll=UNROLL)
            lax.fori_loop(0, 3, functools.partial(apply, half=half), 0, unroll=3)
            for k in range(4):
                swap(p, half, k).start()

    for p in range(3):
        for half in range(2):
            for k in range(4):
                swap(p, half, k).wait()


def per_device(
    pair,
    ln_gain,
    ln_shift,
    proj_weight,
    proj_bias,
    gate_weight,
    gate_bias,
    out_gain,
    out_shift,
    out_weight,
    out_bias,
):
    line = lambda v: v.reshape(1, -1)
    operands = (
        pair,
        line(ln_gain),
        line(ln_shift),
        proj_weight,
        line(proj_bias),
        gate_weight,
        line(gate_bias),
        line(out_gain),
        line(out_shift),
        out_weight,
        line(out_bias),
    )
    vmem = pl.BlockSpec(memory_space=pltpu.VMEM)
    dma = pltpu.SemaphoreType.DMA
    return pl.pallas_call(
        kernel,
        out_shape=jax.ShapeDtypeStruct(pair.shape, BF16),
        in_specs=[pl.BlockSpec(memory_space=pl.ANY)] * 11,
        out_specs=vmem,
        scratch_shapes=[
            *[pltpu.VMEM(v.shape, v.dtype) for v in operands[1:]],
            pltpu.VMEM((48, 192, 128), BF16),
            pltpu.VMEM((512, 128), BF16),
            pltpu.VMEM((512, 128), F32),
            pltpu.VMEM((48, 192, 128), BF16),
            pltpu.VMEM((48, 96, 128), F32),
            pltpu.VMEM((2, 3, 3, 256, 128), F32),
            pltpu.VMEM((2, 3, 8, 32, 384), BF16),
            pltpu.VMEM((2, 3, 8, 32, 384), BF16),
            pltpu.VMEM((4, 2, 96, 384), BF16),
            pltpu.VMEM((8, 3, 4, 2, 32, 384), BF16),
            pltpu.VMEM((48, 48, 128), BF16),
            pltpu.VMEM((3, 32, 48, 128), BF16),
            pltpu.VMEM((1536, 128), F32),
            pltpu.VMEM((3, 128, 128), F32),
            pltpu.VMEM((1536, 128), BF16),
            pltpu.VMEM((2, 8, 32, 384), BF16),
            pltpu.VMEM((2, 8, 32, 384), BF16),
            dma((10,)),
            dma((3, 2)),
            dma((2,)),
            dma((2,)),
            dma((2,)),
            dma((2,)),
            dma((2, 3)),
            dma((2, 3)),
            dma((2, 3, 3)),
            dma((2, 3, 3)),
            dma((2, 3)),
            dma((2, 3)),
            dma((2,)),
            dma((3,)),
            dma((3, 2, 4)),
            dma((3, 2, 4)),
        ],
        compiler_params=pltpu.CompilerParams(
            collective_id=0, has_side_effects=True, vmem_limit_bytes=VMEM_MIB * 1024 * 1024
        ),
    )(*[pltpu.with_memory_space_constraint(v, pltpu.HBM) for v in operands])


def solution(mesh):
    in_specs = (P("row", "col", None),) + (P(),) * 10
    return jax.shard_map(
        per_device, mesh=mesh, in_specs=in_specs, out_specs=P("row", "col", None), check_vma=False
    )
```

```python
import functools

import jax
import jax.numpy as jnp
from jax import lax
from jax.experimental import pallas as pl
from jax.experimental.pallas import tpu as pltpu
from jax.sharding import PartitionSpec as P

F32 = jnp.float32
BF16 = jnp.bfloat16
EPS = 1e-05
NT = (((1,), (1,)), ((), ()))
VMEM_MIB = 50
UNROLL = 6
ORDER = (1, 2, 0)


def remote(src, dst, send_sem, recv_sem, row, col, depth):
    return pltpu.make_async_remote_copy(
        src_ref=src,
        dst_ref=dst,
        send_sem=send_sem,
        recv_sem=recv_sem,
        device_id=(row, col, depth),
        device_id_type=pl.DeviceIdType.MESH,
    )


def kernel(*refs):
    work(refs[0], refs[1:11], refs[12:22], refs[11], *refs[12:])


def work(
    pair_hbm,
    sources,
    params,
    out,
    ln_gain,
    ln_shift,
    proj_weight,
    proj_bias,
    gate_weight,
    gate_bias,
    out_gain,
    out_shift,
    out_weight,
    out_bias,
    pair,
    wt,
    bt,
    normed,
    gate,
    stage,
    sbuf,
    rbuf,
    left,
    ring,
    tsend,
    trecv,
    wide,
    table,
    normal,
    raw,
    raw_in,
    w_sem,
    p_sem,
    w_send,
    w_recv,
    v_send,
    v_recv,
    x_send,
    x_recv,
    r_send,
    r_recv,
    h_send,
    h_recv,
    t_send,
    t_recv,
    o_send,
    o_recv,
):
    row = lax.axis_index("row")
    x = lax.axis_index("col")
    d = lax.axis_index("depth")
    z = row // 2
    yh = row % 2
    yl = d // 2
    core = d % 2
    me = x * 2 + yh

    def load(p, half):
        rows = pl.ds(half * 24 + p * 8, 8)
        return pltpu.make_async_copy(pair_hbm.at[rows], pair.at[rows], p_sem.at[p, half])

    for half in range(2):
        load(0, half).start()
    fetches = [
        pltpu.make_async_copy(src, dst, w_sem.at[n])
        for n, (src, dst) in enumerate(zip(sources, params))
    ]
    for fetch in fetches:
        fetch.start()
    for p in range(1, 3):
        for half in range(2):
            load(p, half).start()

    barrier = pltpu.get_barrier_semaphore()

    up = (row + 2) % 16
    down = (row + 14) % 16
    greeted = [
        (z * 2 + (yh + a) % 2, (x + b) % 4, (d + e) % 4)
        for b in (2, 1, 3, 0)
        for a in (1, 0)
        for e in (2, 1, 3, 0)
        if a or b or e
    ]
    for device in greeted + [(up, x, d), (down, x, d)]:
        pl.semaphore_signal(
            barrier, inc=1, device_id=device, device_id_type=pl.DeviceIdType.MESH
        )

    for fetch in fetches:
        fetch.wait()

    for b in range(4):
        wt[b * 128 : (b + 1) * 128, :] = (
            proj_weight[:, b * 128 : (b + 1) * 128].astype(F32).T.astype(BF16)
        )
        bt[b * 128 : (b + 1) * 128, :] = jnp.broadcast_to(
            proj_bias[:, b * 128 : (b + 1) * 128], (128, 128)
        ).T
    first = pl.multiple_of(d * 32, 32)
    wsel = jnp.concatenate([wt[pl.ds(first + 128 * b, 32), :] for b in range(4)], axis=0)
    gain = ln_gain[...]
    shift = ln_shift[...]

    def project(p):
        def body(n, carry):
            t = p * 8 + n
            vals = jnp.concatenate([pair[t], pair[t + 24]], axis=0).astype(F32)
            centred = vals - jnp.mean(vals, axis=-1, keepdims=True)
            spread = jnp.mean(centred * centred, axis=-1, keepdims=True)
            rows = (centred * lax.rsqrt(spread + EPS) * gain + shift).astype(BF16)
            normed[t] = rows[:192]
            normed[t + 24] = rows[192:]
            mixed = lax.dot_general(wsel, rows, NT, preferred_element_type=F32)
            at = pl.ds(pl.multiple_of(n * 32, 32), 32)
            for q in range(3):
                cut = [
                    mixed[b * 32 : (b + 1) * 32, q * 128 : (q + 1) * 128]
                    + bt[pl.ds(first + 128 * b, 32), :]
                    for b in range(4)
                ]
                stage[0, p, q, at, :] = jax.nn.sigmoid(cut[2]) * cut[3]
                stage[1, p, q, at, :] = jax.nn.sigmoid(cut[0]) * cut[1]
            return carry

        for half in range(2):
            load(p, half).wait()
        lax.fori_loop(0, 8, body, 0, unroll=2)

    def pack(kind, p):
        def body(g, carry):
            for q in range(3):
                rows = [
                    stage[kind, p, q, pl.ds(g * 4 + c, 8, stride=32), :] for c in range(4)
                ]
                sbuf[kind, p, g, :, q * 128 : (q + 1) * 128] = jnp.concatenate(
                    rows, axis=0
                ).astype(BF16)
            return carry

        lax.fori_loop(0, 8, body, 0, unroll=2)

    def spread(source, target, send_sem, recv_sem):
        for n in (5, 4, 3, 1, 2, 6, 7):
            g = (me + n) % 8
            remote(
                source.at[g], target.at[me], send_sem, recv_sem, z * 2 + g % 2, g // 2, d
            ).start()
        pltpu.make_async_copy(source.at[me], target.at[me], recv_sem).start()

    def exchange(kind, p):
        spread(sbuf.at[kind, p], rbuf.at[kind, p], x_send.at[kind, p], x_recv.at[kind, p])

    def raw_copy(way):
        to = up if way == 0 else down
        return remote(sbuf.at[0, 0], raw.at[way], w_send.at[way], w_recv.at[way], to, x, d)

    def raw_spread(way):
        raw_copy(way).wait_recv()
        spread(raw.at[way], raw_in.at[way], v_send.at[way], v_recv.at[way])

    low = lax.broadcasted_iota(jnp.int32, (32, 128), 1) < 64

    def unpack(source, recv_sem, put):
        pltpu.make_async_copy(source, source, recv_sem).wait()
        for u in range(2):
            for y in range(2):
                one = source[4 * u + y].astype(F32)
                two = source[4 * u + 2 + y].astype(F32)
                a = [one[:, q * 128 : (q + 1) * 128] for q in range(3)]
                b = [two[:, q * 128 : (q + 1) * 128] for q in range(3)]
                ra1 = pltpu.roll(a[1], 64, 1)
                ra2 = pltpu.roll(a[2], 64, 1)
                rb0 = pltpu.roll(b[0], 64, 1)
                rb1 = pltpu.roll(b[1], 64, 1)
                evens = [a[0], jnp.where(low, a[1], rb0), jnp.where(low, rb0, rb1)]
                odds = [jnp.where(low, ra1, ra2), jnp.where(low, ra2, b[1]), b[2]]
                for c in range(4):
                    at = slice(c * 8, c * 8 + 8)
                    for q in range(3):
                        put(
                            c, u, y, slice(q * 128, q * 128 + 128),
                            jnp.concatenate([evens[q][at], odds[q][at]], axis=0).astype(BF16),
                        )

    def unpack_right(p):
        def put(c, u, y, lanes, tile):
            ring[z, p, c, u, y * 16 : y * 16 + 16, lanes] = tile

        unpack(rbuf.at[0, p], x_recv.at[0, p], put)

    def unpack_raw(way):
        plane = (z + 7) % 8 if way == 0 else (z + 1) % 8

        def put(c, u, y, lanes, tile):
            ring[plane, 0, c, u, y * 16 : y * 16 + 16, lanes] = tile

        unpack(raw_in.at[way], v_recv.at[way], put)

    def unpack_left(p):
        def put(c, u, y, lanes, tile):
            left[c, u, p * 32 + y * 16 : p * 32 + y * 16 + 16, lanes] = tile

        unpack(rbuf.at[1, p], x_recv.at[1, p], put)

    def ring_copy(way, step, p):
        held = (z + 8 - step + 1) % 8 if way == 0 else (z + step - 1) % 8
        to = up if way == 0 else down
        if step < 4:
            piece = ring.at[held, p]
            return remote(
                piece, piece, r_send.at[way, step - 1, p], r_recv.at[way, step - 1, p], to, x, d
            )
        piece = ring.at[held, p, pl.ds(way * 2, 2)]
        return remote(piece, piece, h_send.at[way, p], h_recv.at[way, p], to, x, d)

    lane_group = lax.broadcasted_iota(jnp.int32, (96, 128), 1) // 32

    def multiply(plane, p):
        tile = None
        for c in range(4):
            total = None
            for u in range(2):
                rows = ring[plane, p, c, u]
                term = lax.dot_general(
                    left[c, u],
                    jnp.concatenate([rows] * 4, axis=0),
                    NT,
                    preferred_element_type=F32,
                )
                total = term if total is None else total + term
            tile = total if tile is None else jnp.where(lane_group == c, total, tile)
        tile = tile.astype(BF16)
        for ph in range(2):
            tsend[(plane * 3 + p) * 2 + ph] = jnp.concatenate(
                [tile[k * 32 + ph * 16 : k * 32 + ph * 16 + 16] for k in range(3)], axis=0
            )
        hand_out(plane, p)

    def hand_out(plane, p):
        pcol = plane // 2
        pcore = plane % 2
        slot = d * 8 + me
        for ph in range(2):
            for rel in range(2):
                prow = z * 2 + ph
                pd = ((yl + rel) % 2) * 2 + pcore
                unit = tsend.at[(plane * 3 + p) * 2 + ph]
                copy = remote(
                    unit, trecv.at[p, slot], t_send.at[rel], t_recv.at[p], prow, pcol, pd
                )
                if rel == 1:
                    copy.start()
                    continue
                other = jnp.logical_or(prow != row, jnp.logical_or(pcol != x, pd != d))

                @pl.when(other)
                def _():
                    copy.start()

                @pl.when(jnp.logical_not(other))
                def _():
                    pltpu.make_async_copy(unit, trecv.at[p, slot], t_recv.at[p]).start()

    def start_ring(p):
        ring_copy(0, 1, p).start()
        ring_copy(1, 1, p).start()

    project(0)
    pack(0, 0)
    project(1)
    pack(0, 1)
    pl.semaphore_wait(barrier, 33)
    exchange(0, 1)
    raw_copy(0).start()
    raw_copy(1).start()
    project(2)
    pack(0, 2)
    exchange(0, 2)
    pack(1, 0)
    exchange(1, 0)
    pack(1, 1)
    exchange(1, 1)
    pack(1, 2)
    unpack_right(1)
    start_ring(1)
    raw_spread(0)
    raw_spread(1)
    unpack_right(2)
    start_ring(2)
    exchange(1, 2)
    exchange(0, 0)

    mine = pl.ds(pl.multiple_of(core * 96, 96), 96)

    def gate_rows(n, carry):
        at = pl.ds(n * 4, 4)
        logits = (
            jnp.dot(
                normed[at, mine, :].reshape(384, 128),
                gate_weight[...],
                preferred_element_type=F32,
            )
            + gate_bias[...]
        )
        gate[at] = jax.nn.sigmoid(logits).reshape(4, 96, 128)
        return carry

    lax.fori_loop(0, 12, gate_rows, 0)
    table[0] = jnp.broadcast_to(out_gain[...], (128, 128)).T
    table[1] = jnp.broadcast_to(out_shift[...], (128, 128)).T
    table[2] = out_weight[...].astype(F32)

    for step in range(1, 5):
        plus = (z + 8 - step) % 8
        minus = (z + step) % 8
        for p in ORDER:
            for way in range(2):
                if step == 1 and p == 0:
                    unpack_raw(way)
                else:
                    ring_copy(way, step, p).wait_recv()
                if step < 4:
                    ring_copy(way, step + 1, p).start()
            if step == 2:
                multiply((z + 7) % 8, p)
                multiply((z + 1) % 8, p)
            if step > 1:
                multiply(plus, p)
                if step < 4:
                    multiply(minus, p)
        if step == 1:
            unpack_right(0)
            for p in range(3):
                unpack_left(p)
            for p in range(3):
                multiply(z, p)

    def regroup(n):
        return jnp.concatenate(
            [table[n, pl.ds(c, 32, stride=4), :] for c in range(4)], axis=0
        )

    gains = regroup(0)
    shifts = regroup(1)
    weight = regroup(2).astype(BF16)
    group = lax.broadcasted_iota(jnp.int32, (32, 128), 1) // 32

    def swap(p, half, k):
        columns = pl.ds(pl.multiple_of(core * 96 + k * 24 + p * 8, 8), 8)
        piece = out.at[pl.ds(half * 24, 24), columns, :]
        return remote(
            piece,
            piece,
            o_send.at[p, half, k],
            o_recv.at[p, half, k],
            row,
            x,
            yl * 2 + 1 - core,
        )

    def drain():
        for kind in range(2):
            for p in range(3):
                pltpu.make_async_copy(
                    sbuf.at[kind, p, pl.ds(0, 7)], rbuf.at[kind, p, pl.ds(0, 7)], x_send.at[kind, p]
                ).wait()
        for way in range(2):
            raw_copy(way).wait_send()
            pltpu.make_async_copy(
                raw.at[way, pl.ds(0, 7)], raw_in.at[way, pl.ds(0, 7)], v_send.at[way]
            ).wait()
        for step in range(1, 5):
            for p in range(3):
                for way in range(2):
                    if step > 1 or p > 0:
                        ring_copy(way, step, p).wait_send()
        for rel in range(2):
            units = tsend.at[pl.ds(0, 45 if rel == 0 else 48)]
            pltpu.make_async_copy(units, units, t_send.at[rel]).wait()

    for p in ORDER:
        if p == ORDER[2]:
            drain()
        pltpu.make_async_copy(trecv.at[p], trecv.at[p], t_recv.at[p]).wait()

        def widen(s, carry, p=p):
            at = pl.ds(pl.multiple_of(s * 192, 192), 192)
            wide[at, :] = trecv[p, pl.ds(s * 4, 4)].reshape(192, 128).astype(F32)
            return carry

        lax.fori_loop(0, 8, widen, 0, unroll=2)

        def finish(n, carry, half):
            g = (n // 2) * 4 + half * 2 + n % 2
            from_row = [wide[pl.ds(g * 4 + i, 32, stride=48), :] for i in range(4)]
            blocks = []
            for c in range(4):
                block = None
                for i in range(4):
                    turn = (32 * (i - c)) % 128
                    moved = pltpu.roll(from_row[i], turn, 1) if turn else from_row[i]
                    block = moved if block is None else jnp.where(group == i, moved, block)
                blocks.append(block)
            vals = jnp.concatenate(blocks, axis=0)
            centred = vals - jnp.mean(vals, axis=0, keepdims=True)
            spread = jnp.mean(centred * centred, axis=0, keepdims=True)
            rows = (centred * lax.rsqrt(spread + EPS) * gains + shifts).astype(BF16)
            at = pl.ds(pl.multiple_of(half * 768 + n * 128, 128), 128)
            normal[at, :] = rows.T
            return carry

        def apply(n, carry, half, p=p):
            rows = normal[pl.ds(pl.multiple_of(half * 768 + n * 256, 256), 256), :]
            projected = jnp.dot(rows, weight, preferred_element_type=F32) + out_bias[...]
            for i in range(8):
                line = half * 24 + n * 8 + i
                for k in range(4):
                    j = k * 24 + p * 8
                    value = (
                        gate[line, j : j + 8, :]
                        * projected[i * 32 + k * 8 : i * 32 + k * 8 + 8]
                    )
                    out[line, pl.ds(pl.multiple_of(core * 96 + j, 8), 8), :] = value.astype(BF16)
            return carry

        for half in range(2):
            lax.fori_loop(0, 6, functools.partial(finish, half=half), 0, unroll=UNROLL)
            lax.fori_loop(0, 3, functools.partial(apply, half=half), 0, unroll=3)
            for k in range(4):
                swap(p, half, k).start()

    for p in range(3):
        for half in range(2):
            for k in range(4):
                swap(p, half, k).wait()


def per_device(
    pair,
    ln_gain,
    ln_shift,
    proj_weight,
    proj_bias,
    gate_weight,
    gate_bias,
    out_gain,
    out_shift,
    out_weight,
    out_bias,
):
    line = lambda v: v.reshape(1, -1)
    operands = (
        pair,
        line(ln_gain),
        line(ln_shift),
        proj_weight,
        line(proj_bias),
        gate_weight,
        line(gate_bias),
        line(out_gain),
        line(out_shift),
        out_weight,
        line(out_bias),
    )
    vmem = pl.BlockSpec(memory_space=pltpu.VMEM)
    dma = pltpu.SemaphoreType.DMA
    return pl.pallas_call(
        kernel,
        out_shape=jax.ShapeDtypeStruct(pair.shape, BF16),
        in_specs=[pl.BlockSpec(memory_space=pl.ANY)] * 11,
        out_specs=vmem,
        scratch_shapes=[
            *[pltpu.VMEM(v.shape, v.dtype) for v in operands[1:]],
            pltpu.VMEM((48, 192, 128), BF16),
            pltpu.VMEM((512, 128), BF16),
            pltpu.VMEM((512, 128), F32),
            pltpu.VMEM((48, 192, 128), BF16),
            pltpu.VMEM((48, 96, 128), F32),
            pltpu.VMEM((2, 3, 3, 256, 128), F32),
            pltpu.VMEM((2, 3, 8, 32, 384), BF16),
            pltpu.VMEM((2, 3, 8, 32, 384), BF16),
            pltpu.VMEM((4, 2, 96, 384), BF16),
            pltpu.VMEM((8, 3, 4, 2, 32, 384), BF16),
            pltpu.VMEM((48, 48, 128), BF16),
            pltpu.VMEM((3, 32, 48, 128), BF16),
            pltpu.VMEM((1536, 128), F32),
            pltpu.VMEM((3, 128, 128), F32),
            pltpu.VMEM((1536, 128), BF16),
            pltpu.VMEM((2, 8, 32, 384), BF16),
            pltpu.VMEM((2, 8, 32, 384), BF16),
            dma((10,)),
            dma((3, 2)),
            dma((2,)),
            dma((2,)),
            dma((2,)),
            dma((2,)),
            dma((2, 3)),
            dma((2, 3)),
            dma((2, 3, 3)),
            dma((2, 3, 3)),
            dma((2, 3)),
            dma((2, 3)),
            dma((2,)),
            dma((3,)),
            dma((3, 2, 4)),
            dma((3, 2, 4)),
        ],
        compiler_params=pltpu.CompilerParams(
            collective_id=0, has_side_effects=True, vmem_limit_bytes=VMEM_MIB * 1024 * 1024
        ),
    )(*[pltpu.with_memory_space_constraint(v, pltpu.HBM) for v in operands])


def solution(mesh):
    in_specs = (P("row", "col", None),) + (P(),) * 10
    return jax.shard_map(
        per_device, mesh=mesh, in_specs=in_specs, out_specs=P("row", "col", None), check_vma=False
    )
```
